128 devices in a mesh: m: 1, kk: 16 (over z, y), g: 8 (over x, core).
Axes of the slice: x: 4, y: 4, z: 4, core: 2. Of those that a mesh axis runs over, the one named last changes fastest.
Arguments:
- a_mat: bfloat16 [8192, 8192], P(('m', 'g'), 'kk')
Outputs:
- output: float32 [8, 5, 1024, 1024], P(('m', 'g'), None, 'kk')
All inputs are finite; a program needn't handle non-finite values.
Results may differ from the reference program's by a relative error of at most 0.001.
Values are sent between devices in bfloat16 or wider.
A program may use at most 1 GiB of HBM per device.

```python
import math
import jax
import jax.numpy as jnp
from jax import lax

N_ROWS = 8192
K_COLS = 8192
GROUP_SIZE = 8

BLOCK_ROWS = N_ROWS // GROUP_SIZE
SLOT_COUNT = GROUP_SIZE // 2 + 1


def pair_table(groups):
    half_size = groups // 2
    step_width = max(1, math.isqrt(half_size))
    left_tab = []
    right_tab = []
    for dev_pos in range(groups):
        left_tab.append(dev_pos)
        right_tab.append(dev_pos)
        for diff_pos in range(1, half_size + 1):
            big_off = -(-diff_pos // step_width) * step_width
            if 2 * diff_pos == groups and dev_pos >= half_size:
                left_tab.append(-1)
                right_tab.append(-1)
            else:
                left_tab.append((dev_pos + big_off) % groups)
                right_tab.append((dev_pos + big_off - diff_pos) % groups)
    return left_tab, right_tab


def setup_inputs(seed: int = 0, part: int = 0) -> dict:
    base_key = jax.random.fold_in(jax.random.key(seed), part)
    key_val, key_scale = jax.random.split(base_key)
    values = jax.random.normal(key_val, (GROUP_SIZE, BLOCK_ROWS, K_COLS), jnp.float32)
    block_scale = jax.random.uniform(key_scale, (GROUP_SIZE, 1, 1), jnp.float32, 0.7, 1.4)
    a_mat = (values * block_scale).reshape(N_ROWS, K_COLS) * (K_COLS ** -0.25)
    return {"a_mat": a_mat.astype(jnp.bfloat16)}


def reference(a_mat):
    left_tab, right_tab = pair_table(GROUP_SIZE)
    pair_idx = jnp.array([[max(left_val, 0), max(right_val, 0)] for left_val, right_val in zip(left_tab, right_tab)], dtype=jnp.int32)
    keep_slot = jnp.array([left_val >= 0 for left_val in left_tab])
    blocks = a_mat.reshape(GROUP_SIZE, BLOCK_ROWS, K_COLS)

    def one_block(pair_row):
        row_blk = lax.dynamic_index_in_dim(blocks, pair_row[0], 0, keepdims=False)
        col_blk = lax.dynamic_index_in_dim(blocks, pair_row[1], 0, keepdims=False)
        return jnp.dot(row_blk, col_blk.T, preferred_element_type=jnp.float32)

    products = lax.map(one_block, pair_idx)
    products = jnp.where(keep_slot[:, None, None], products, 0.0)
    return products.reshape(GROUP_SIZE, SLOT_COUNT, BLOCK_ROWS, BLOCK_ROWS)
```

```python
import functools
import jax
import jax.numpy as jnp
from jax import lax
from jax.experimental import pallas as pl
from jax.experimental.pallas import tpu as pltpu
from jax.sharding import PartitionSpec as P

MESH = pl.DeviceIdType.MESH
DELTA = (0, 1, 3, 2)


def kernel(a_hbm, out_ref, full, chunk, part, sum1, sum2, mine, theirs, ssem, rsem, lsem):
    kk, p = lax.axis_index("kk"), lax.axis_index("g")
    z, y = kk // 4, kk % 4
    rows, cols = a_hbm.shape
    quarter, half, strip = rows // 4, rows // 8, rows // 16

    zp, zm = {"kk": (z + 1) % 4 * 4 + y}, {"kk": (z + 3) % 4 * 4 + y}
    yp, ym = {"kk": z * 4 + (y + 1) % 4}, {"kk": z * 4 + (y + 3) % 4}
    gp, gm = {"g": (p + 1) % 8}, {"g": (p + 7) % 8}
    far = {"g": (p + 4) % 8}
    odd = p % 2 == 1
    low = p < 4

    own = pltpu.make_async_copy(a_hbm, full.at[:, pl.ds(0, cols)], lsem)
    own.start()
    barrier = pltpu.get_barrier_semaphore()
    for dev in (zp, zm, yp, ym, gp, gm):
        pl.semaphore_signal(barrier, inc=1, device_id=dev, device_id_type=MESH)

    @pl.when(odd)
    def _():
        pl.semaphore_signal(barrier, inc=1, device_id=far, device_id_type=MESH)

    pl.semaphore_wait(barrier, 6 + p % 2)
    own.wait()

    count = [0]
    sent = []

    def slot():
        count[0] += 1
        return count[0] - 1

    def copy(src, dst, dev, idx=None):
        i = slot() if idx is None else idx
        return pltpu.make_async_remote_copy(
            src_ref=src, dst_ref=dst, send_sem=ssem.at[i], recv_sem=rsem.at[i],
            device_id=dev, device_id_type=MESH)

    def send(src, dst, dev):
        c = copy(src, dst, dev)
        c.start()
        sent.append(c)
        return c

    def q(d):
        return pl.multiple_of((z + d) % 4 * quarter, quarter)

    def shard(start, size, r):
        return full.at[pl.ds(start, size), pl.ds(r * cols, cols)]

    def zplus(start, size, r_src):
        return send(shard(start, size, r_src), shard(start, size, (r_src + 3) % 4), zp)

    def zminus(start, size, r_src):
        return send(shard(start, size, r_src), shard(start, size, (r_src + 1) % 4), zm)

    far_idx = [slot() for _ in range(4)]

    def piece(j, r):
        if j == 0:
            return shard(q(0), quarter, r)
        return chunk.at[j - 1, :, pl.ds(r * cols, cols)]

    def far_copy(j, r, dev):
        return copy(piece(j, r), piece(4, r), dev, far_idx[r])

    passed = {}

    def pass_on(j, r):
        passed[j, r] = send(piece(j, r), piece(j + 1, r), gm)
        if j == 0:
            @pl.when(odd & ~low)
            def _():
                far_copy(0, r, far).start()

    pass_on(0, 0)
    m1, p1 = zplus(q(1), quarter, 0), zminus(q(3), quarter, 0)
    m2, p2 = zplus(q(2), half, 0), zminus(q(2) + half, half, 0)
    m1.wait_recv()
    pass_on(0, 3)
    p1.wait_recv()
    pass_on(0, 1)
    m2.wait_recv()
    m3 = zplus(q(1), half, 3)
    p2.wait_recv()
    p3 = zminus(q(3) + half, half, 1)
    m4, p4 = zplus(q(2) + half, half, 0), zminus(q(2), half, 0)
    m9, p9 = zplus(q(0), quarter, 3), zminus(q(0), quarter, 1)
    m7, p7 = zplus(q(0), quarter, 0), zminus(q(0), quarter, 0)
    m5, p5 = zplus(q(3), quarter, 0), zminus(q(1), quarter, 0)

    def strip_rows(d):
        return pl.ds(pl.multiple_of((y + d) % 4 * strip, strip), strip)

    def product(j, d0, n):
        for d in range(d0, d0 + n):
            left = full[pl.ds(q(0), quarter), :] if j == 0 else chunk[j - 1]
            part[j, :, pl.ds(d * quarter, quarter)] = lax.dot_general(
                left, full[pl.ds(q(DELTA[d]), quarter), :],
                (((1,), (1,)), ((), ())), preferred_element_type=jnp.float32)

    def unit(j, d0, n):
        c0, width = d0 * quarter, n * quarter
        hw = width // 2
        u = {}
        lo, hi, whole = pl.ds(c0, hw), pl.ds(c0 + hw, hw), pl.ds(c0, width)
        land = pl.ds(c0 // 2, hw)
        u["a"] = copy(part.at[j, strip_rows(2), lo], sum1.at[0, j, :, land], yp)
        u["b"] = copy(part.at[j, strip_rows(2), hi], sum1.at[1, j, :, land], ym)
        u["c"] = copy(part.at[j, strip_rows(1), whole], sum2.at[0, j, :, whole], yp)
        u["d"] = copy(part.at[j, strip_rows(3), whole], sum2.at[1, j, :, whole], ym)

        def begin():
            product(j, d0, n)
            u["a"].start()
            u["b"].start()

        def middle():
            u["a"].wait_recv()
            part[j, strip_rows(1), lo] += sum1[0, j, :, land]
            u["c"].start()
            u["b"].wait_recv()
            part[j, strip_rows(3), hi] += sum1[1, j, :, land]
            u["d"].start()

        def end():
            u["c"].wait_recv()
            u["d"].wait_recv()
            total = part[j, strip_rows(0), whole] + sum2[0, j, :, whole] + sum2[1, j, :, whole]
            if j % 2 == 0:
                for d in range(d0, d0 + n):
                    out_ref[j, :, pl.ds(q(DELTA[d]), quarter)] = total[:, (d - d0) * quarter:(d - d0 + 1) * quarter]
            else:
                mine[j // 2, :, whole] = total
                u["e"] = send(mine.at[j // 2, :, whole], theirs.at[j // 2, :, whole], gm)

        def receive():
            u["e"].wait_recv()
            for d in range(d0, d0 + n):
                out_ref[j, :, pl.ds(q(DELTA[d]), quarter)] = theirs[j // 2, :, pl.ds(d * quarter, quarter)]

        def settle():
            for key in "abcd":
                u[key].wait_send()

        return dict(begin=begin, middle=middle, end=end, receive=receive, settle=settle)

    u00, u10 = unit(0, 0, 1), unit(1, 0, 1)
    u01, u11 = unit(0, 1, 2), unit(1, 1, 2)
    u20 = unit(2, 0, 3)
    u02, u12, u22 = unit(0, 3, 1), unit(1, 3, 1), unit(2, 3, 1)
    u30, u31 = unit(3, 0, 2), unit(3, 2, 2)
    u40, u41 = unit(4, 0, 2), unit(4, 2, 2)

    m3.wait_recv()
    p3.wait_recv()
    pass_on(0, 2)
    u00["begin"]()
    for r in (0, 3, 1, 2):
        passed[0, r].wait_recv()
        pass_on(1, r)
    u10["begin"]()
    u00["middle"]()
    m4.wait_recv()
    p4.wait_recv()
    m9.wait_recv()
    p9.wait_recv()
    m7.wait_recv()
    m8 = zplus(q(3), half, 3)
    p7.wait_recv()
    p8 = zminus(q(1) + half, half, 1)
    u10["middle"]()
    u01["begin"]()
    u11["begin"]()
    for r in (0, 3, 1, 2):
        passed[1, r].wait_recv()
        pass_on(2, r)
    u01["middle"]()
    u20["begin"]()
    u11["middle"]()
    u00["end"]()
    u10["end"]()
    m5.wait_recv()
    p5.wait_recv()
    u20["middle"]()
    m8.wait_recv()
    p8.wait_recv()
    u02["begin"]()
    u12["begin"]()
    u22["begin"]()
    for r in (0, 3, 1, 2):
        passed[2, r].wait_recv()

        @pl.when(odd & low)
        def _():
            far_copy(3, r, gm).start()

    u30["begin"]()
    u02["middle"]()
    u12["middle"]()
    u22["middle"]()
    u31["begin"]()
    u30["middle"]()
    u01["end"]()
    u11["end"]()
    u31["middle"]()

    @pl.when(low)
    def _():
        for r in (0, 3, 1, 2):
            far_copy(0, r, far).wait_recv()
        u40["begin"]()
        u41["begin"]()

    u20["end"]()
    u02["end"]()
    u12["end"]()
    u22["end"]()

    @pl.when(low)
    def _():
        u40["middle"]()
        u41["middle"]()

    u30["end"]()
    u31["end"]()
    for u in (u10, u11, u12):
        u["receive"]()

    @pl.when(low)
    def _():
        u40["end"]()
        u41["end"]()

    @pl.when(~low)
    def _():
        out_ref[4] = jnp.zeros(out_ref.shape[1:], out_ref.dtype)

    u30["receive"]()
    u31["receive"]()

    for c in sent:
        c.wait_send()
    for u in (u00, u10, u01, u11, u20, u02, u12, u22, u30, u31):
        u["settle"]()

    @pl.when(low)
    def _():
        u40["settle"]()
        u41["settle"]()

    @pl.when(odd)
    def _():
        for r in range(4):
            far_copy(0, r, far).wait_send()


def solution(mesh):
    def local_fn(a_blk):
        rows, cols = a_blk.shape
        strip = rows // 16
        out = pl.pallas_call(
            kernel,
            out_shape=jax.ShapeDtypeStruct((5, strip, rows), jnp.float32),
            in_specs=[pl.BlockSpec(memory_space=pltpu.HBM)],
            out_specs=pl.BlockSpec(memory_space=pltpu.VMEM),
            scratch_shapes=[
                pltpu.VMEM((rows, 4 * cols), jnp.bfloat16),
                pltpu.VMEM((4, rows // 4, 4 * cols), jnp.bfloat16),
                pltpu.VMEM((5, rows // 4, rows), jnp.float32),
                pltpu.VMEM((2, 5, strip, rows // 2), jnp.float32),
                pltpu.VMEM((2, 5, strip, rows), jnp.float32),
                pltpu.VMEM((2, strip, rows), jnp.float32),
                pltpu.VMEM((2, strip, rows), jnp.float32),
                pltpu.SemaphoreType.DMA((112,)),
                pltpu.SemaphoreType.DMA((112,)),
                pltpu.SemaphoreType.DMA,
            ],
            compiler_params=pltpu.CompilerParams(
                collective_id=0, has_side_effects=True, vmem_limit_bytes=48 * 1024 * 1024),
        )(a_blk)
        return out[None]

    return jax.shard_map(local_fn, mesh=mesh, in_specs=(P(("m", "g"), "kk"),), out_specs=P(("m", "g"), None, "kk", None), check_vma=False)
```

```python
import functools
import jax
import jax.numpy as jnp
from jax import lax
from jax.experimental import pallas as pl
from jax.experimental.pallas import tpu as pltpu
from jax.sharding import PartitionSpec as P

MESH = pl.DeviceIdType.MESH
DELTA = (0, 1, 3, 2)


def kernel(a_hbm, out_ref, full, chunk, part, sum1, sum2, mine, theirs, ssem, rsem, lsem, gate):
    kk, p = lax.axis_index("kk"), lax.axis_index("g")
    z, y = kk // 4, kk % 4
    rows, cols = a_hbm.shape
    quarter, half, strip = rows // 4, rows // 8, rows // 16

    zp, zm = {"kk": (z + 1) % 4 * 4 + y}, {"kk": (z + 3) % 4 * 4 + y}
    yp, ym = {"kk": z * 4 + (y + 1) % 4}, {"kk": z * 4 + (y + 3) % 4}
    gp, gm = {"g": (p + 1) % 8}, {"g": (p + 7) % 8}
    next_chip, last_chip = {"g": (p + 2) % 8}, {"g": (p + 6) % 8}
    odd = p % 2 == 1
    low = p < 4

    own = pltpu.make_async_copy(a_hbm, full.at[:, pl.ds(0, cols)], lsem)
    own.start()
    barrier = pltpu.get_barrier_semaphore()
    for dev in (zp, zm, yp, ym, gp, gm):
        pl.semaphore_signal(barrier, inc=1, device_id=dev, device_id_type=MESH)

    @pl.when(odd)
    def _():
        pl.semaphore_signal(barrier, inc=1, device_id=next_chip, device_id_type=MESH)
        pl.semaphore_signal(barrier, inc=1, device_id=last_chip, device_id_type=MESH)

    pl.semaphore_wait(barrier, 6 + p % 2 * 2)
    own.wait()

    slots = iter(range(ssem.shape[0]))

    def copy(src, dst, dev):
        i = next(slots)
        return pltpu.make_async_remote_copy(
            src_ref=src, dst_ref=dst, send_sem=ssem.at[i], recv_sem=rsem.at[i],
            device_id=dev, device_id_type=MESH)

    def start(*copies):
        for c in copies:
            c.start()

    def arrived(*copies):
        for c in copies:
            c.wait_recv()

    def left(*copies):
        for c in copies:
            c.wait_send()

    def q(d):
        return pl.multiple_of((z + d) % 4 * quarter, quarter)

    def shard(first, size, r):
        return full.at[pl.ds(first, size), pl.ds(r * cols, cols)]

    def zplus(first, size, r):
        return copy(shard(first, size, r), shard(first, size, (r + 3) % 4), zp)

    def zminus(first, size, r):
        return copy(shard(first, size, r), shard(first, size, (r + 1) % 4), zm)

    m1, p1 = zplus(q(1), quarter, 0), zminus(q(3), quarter, 0)
    m2, p2 = zplus(q(2), half, 0), zminus(q(2) + half, half, 0)
    m3, p3 = zplus(q(1), half, 3), zminus(q(3) + half, half, 1)
    m4, p4 = zplus(q(2) + half, half, 0), zminus(q(2), half, 0)
    m9, p9 = zplus(q(0), quarter, 3), zminus(q(0), quarter, 1)
    m7, p7 = zplus(q(0), quarter, 0), zminus(q(0), quarter, 0)
    m5, p5 = zplus(q(3), quarter, 0), zminus(q(1), quarter, 0)
    m8, p8 = zplus(q(3), half, 3), zminus(q(1) + half, half, 1)

    def piece(j, r):
        return shard(q(0), quarter, r) if j == 0 else chunk.at[j - 1, :, pl.ds(r * cols, cols)]

    def leg(src, dst, dev):
        return [copy(piece(src, r), piece(dst, r), dev) for r in range(4)]

    x1, x2, x3 = leg(0, 1, gm), leg(1, 2, gm), leg(2, 3, gm)
    y1, y2, x4 = leg(0, 5, next_chip), leg(5, 4, next_chip), leg(3, 4, gm)
    ARRIVAL = (0, 3, 1, 2)

    def own_piece(r):
        x1[r].start()

        @pl.when(odd)
        def _():
            y1[r].start()

    def forward(got, give, shards=ARRIVAL):
        for r in shards:
            got[r].wait_recv()
            give[r].start()

    def strip_rows(d):
        return pl.ds(pl.multiple_of((y + d) % 4 * strip, strip), strip)

    class Unit:
        def __init__(self, j, d0, n):
            step = half if j == 4 else quarter
            c0, width = d0 * step, n * step
            hw = width // 2
            self.j, self.ds, self.step = j, range(d0, d0 + n), step
            self.lo, self.hi, self.whole = pl.ds(c0, hw), pl.ds(c0 + hw, hw), pl.ds(c0, width)
            self.land = pl.ds(c0 // 2, hw)
            self.a = copy(part.at[j, strip_rows(2), self.lo], sum1.at[0, j, :, self.land], yp)
            self.b = copy(part.at[j, strip_rows(2), self.hi], sum1.at[1, j, :, self.land], ym)
            self.c = copy(part.at[j, strip_rows(1), self.whole], sum2.at[0, j, :, self.whole], yp)
            self.d = copy(part.at[j, strip_rows(3), self.whole], sum2.at[1, j, :, self.whole], ym)
            if j == 4:
                self.sends = [
                    copy(mine.at[2, :, pl.ds(d * step, step)], theirs.at[2, :, pl.ds(d * step, step)],
                         {"kk": (z + DELTA[d]) % 4 * 4 + y, "g": (p + 4) % 8})
                    for d in self.ds]
            elif j % 2:
                self.sends = [copy(mine.at[j // 2, :, self.whole], theirs.at[j // 2, :, self.whole], gm)]
            else:
                self.sends = []

        def multiply(self, d, lhs, rhs):
            part[self.j, :, pl.ds(d * self.step, self.step)] = lax.dot_general(
                lhs, rhs, (((1,), (1,)), ((), ())), preferred_element_type=jnp.float32)

        def begin(self):
            j = self.j
            for d in self.ds:
                rows_d = pl.ds(q(DELTA[d]), quarter)
                if j == 0:
                    self.multiply(d, full[pl.ds(q(0), quarter), :], full[rows_d, :])
                elif j < 4:
                    self.multiply(d, chunk[j - 1], full[rows_d, :])
                else:
                    @pl.when(low)
                    def _():
                        self.multiply(d, chunk[3], full[pl.ds(q(DELTA[d]), half), :])

                    @pl.when(~low)
                    def _():
                        self.multiply(d, full[rows_d, :], chunk[3, half:])
            start(self.a, self.b)

        def middle(self):
            j = self.j
            self.a.wait_recv()
            part[j, strip_rows(1), self.lo] += sum1[0, j, :, self.land]
            self.c.start()
            self.b.wait_recv()
            part[j, strip_rows(3), self.hi] += sum1[1, j, :, self.land]
            self.d.start()

        def place(self, value):
            for i, d in enumerate(self.ds):
                out_ref[self.j, :, pl.ds(q(DELTA[d]), self.step)] = value[:, i * self.step:(i + 1) * self.step]

        def end(self):
            j = self.j
            arrived(self.c, self.d)
            total = part[j, strip_rows(0), self.whole] + sum2[0, j, :, self.whole] + sum2[1, j, :, self.whole]
            if j == 4:
                @pl.when(low)
                def _():
                    self.place(total)

                @pl.when(~low)
                def _():
                    mine[2, :, self.whole] = total
                    start(*self.sends)
            elif j % 2:
                mine[j // 2, :, self.whole] = total
                start(*self.sends)
            else:
                self.place(total)

        def receive(self):
            arrived(*self.sends)
            if self.j == 4:
                for d in self.ds:
                    first = pl.multiple_of(q(4 - DELTA[d]) + half, half)
                    out_ref[4, :, pl.ds(first, half)] = theirs[2, :, pl.ds(d * half, half)]
            else:
                self.place(theirs[self.j // 2, :, self.whole])

        def settle(self):
            left(self.a, self.b, self.c, self.d)
            if self.j != 4:
                left(*self.sends)

    u00, u10 = Unit(0, 0, 1), Unit(1, 0, 1)
    u01, u11 = Unit(0, 1, 1), Unit(1, 1, 1)
    u20, u21 = Unit(2, 0, 1), Unit(2, 1, 1)
    u02, u12, u22 = Unit(0, 2, 1), Unit(1, 2, 1), Unit(2, 2, 1)
    u03, u13, u23 = Unit(0, 3, 1), Unit(1, 3, 1), Unit(2, 3, 1)
    u30, u31 = Unit(3, 0, 2), Unit(3, 2, 2)
    u40, u41 = Unit(4, 0, 2), Unit(4, 2, 2)
    always = (u00, u10, u01, u11, u20, u21, u02, u12, u22, u03, u13, u23, u30, u31, u40, u41)

    def both(*steps):
        for step in steps:
            step()

    rest = (m9, p9, m7, p4, m5, p5)

    def head():
        start(m2, p2, m1, p1)
        own_piece(0)
        arrived(m2)
        start(m3)
        arrived(p2)
        start(p3)
        pl.when(~odd)(lambda: start(m4, p7))
        forward(x1, x2, shards=(0,))
        arrived(m1)
        own_piece(3)
        arrived(p1)
        own_piece(1)
        pl.when(~odd)(lambda: start(*rest))
        arrived(m3, p3)
        own_piece(2)
        u00.begin()

    def even_core():
        forward(x1, x2, shards=(3, 1, 2))
        u10.begin()
        arrived(m4, p7)
        start(p8)
        arrived(p9)
        both(u01.begin, u11.begin, u00.middle, u10.middle)
        forward(x2, x3, shards=(0, 3))
        arrived(m9, m7)
        start(m8)
        arrived(p4)
        pl.semaphore_signal(gate, inc=1, device_id=gp, device_id_type=MESH)
        both(u02.begin, u12.begin)
        forward(x2, x3, shards=(1, 2))
        both(u20.begin, u21.begin, u22.begin, u01.middle, u11.middle, u02.middle, u12.middle)
        arrived(m5, p5, m8, p8)
        both(u03.begin, u13.begin, u23.begin, u20.middle, u21.middle, u22.middle)
        arrived(*x3)
        both(u30.begin, u31.begin, u03.middle, u13.middle, u23.middle)
        both(u10.end, u11.end, u00.end, u01.end, u30.middle, u31.middle, u12.end)
        arrived(*x4)
        both(u40.begin, u41.begin)
        both(u02.end, u20.end, u21.end, u22.end, u13.end)
        both(u40.middle, u41.middle)
        both(u30.end, u31.end, u40.end, u41.end, u03.end, u23.end)

    def odd_core():
        forward(x1, x2, shards=(3, 1))
        forward(y1, y2, shards=(0, 3))
        pl.semaphore_wait(gate, 1)
        start(m4, p7, *rest)
        forward(x1, x2, shards=(2,))
        both(u10.begin, u00.middle)
        forward(y1, y2, shards=(1, 2))
        u10.middle()
        forward(x2, x3, shards=(0, 3, 1))
        arrived(m4, p7)
        start(p8)
        arrived(p9)
        both(u01.begin, u11.begin)
        forward(x2, x3, shards=(2,))
        both(u20.begin, u21.begin)
        arrived(m9, m7)
        start(m8)
        arrived(p4)
        both(u02.begin, u12.begin, u22.begin, u01.middle, u11.middle, u20.middle, u21.middle)
        arrived(m5, p5, m8, p8, *y2)
        both(u40.begin, u41.begin, u03.begin, u13.begin, u23.begin)
        both(u02.middle, u12.middle, u22.middle, u40.middle, u41.middle)
        forward(x3, x4)
        both(u30.begin, u31.begin, u13.middle, u03.middle, u23.middle)
        both(u10.end, u11.end, u00.end, u01.end, u20.end, u21.end, u12.end, u30.middle, u31.middle)
        both(u40.end, u41.end, u13.end, u02.end, u22.end, u03.end, u23.end, u30.end, u31.end)

    head()
    pl.when(~odd)(even_core)
    pl.when(odd)(odd_core)
    both(u10.receive, u11.receive, u12.receive, u13.receive, u30.receive, u31.receive)

    @pl.when(low)
    def _():
        both(u40.receive, u41.receive)

    @pl.when(~low)
    def _():
        out_ref[4] = jnp.zeros(out_ref.shape[1:], out_ref.dtype)

    left(m1, p1)
    left(m2, p2, m3, p3, m4, p4, m5, p5, m7, p7, m8, p8, m9, p9, *x1, *x2, *x3)
    for u in always:
        u.settle()

    @pl.when(odd)
    def _():
        left(*x4, *y1, *y2)

    @pl.when(~low)
    def _():
        left(*u40.sends, *u41.sends)


def solution(mesh):
    def local_fn(a_blk):
        rows, cols = a_blk.shape
        strip = rows // 16
        out = pl.pallas_call(
            kernel,
            out_shape=jax.ShapeDtypeStruct((5, strip, rows), jnp.float32),
            in_specs=[pl.BlockSpec(memory_space=pltpu.HBM)],
            out_specs=pl.BlockSpec(memory_space=pltpu.VMEM),
            scratch_shapes=[
                pltpu.VMEM((rows, 4 * cols), jnp.bfloat16),
                pltpu.VMEM((5, rows // 4, 4 * cols), jnp.bfloat16),
                pltpu.VMEM((5, rows // 4, rows), jnp.float32),
                pltpu.VMEM((2, 5, strip, rows // 2), jnp.float32),
                pltpu.VMEM((2, 5, strip, rows), jnp.float32),
                pltpu.VMEM((3, strip, rows), jnp.float32),
                pltpu.VMEM((3, strip, rows), jnp.float32),
                pltpu.SemaphoreType.DMA((160,)),
                pltpu.SemaphoreType.DMA((160,)),
                pltpu.SemaphoreType.DMA,
                pltpu.SemaphoreType.REGULAR,
            ],
            compiler_params=pltpu.CompilerParams(
                collective_id=0, has_side_effects=True, vmem_limit_bytes=48 * 1024 * 1024),
        )(a_blk)
        return out[None]

    return jax.shard_map(local_fn, mesh=mesh, in_specs=(P(("m", "g"), "kk"),), out_specs=P(("m", "g"), None, "kk", None), check_vma=False)
```

```python
import functools
import jax
import jax.numpy as jnp
from jax import lax
from jax.experimental import pallas as pl
from jax.experimental.pallas import tpu as pltpu
from jax.sharding import PartitionSpec as P

MESH = pl.DeviceIdType.MESH
DELTA = (0, 1, 3, 2)


def kernel(a_hbm, a_strips, out_ref, full, fully, chunk, chunky, part, sum1, sum2, mine, theirs, ssem, rsem, lsem, lsem2, gate):
    kk, p = lax.axis_index("kk"), lax.axis_index("g")
    z, y = kk // 4, kk % 4
    rows, cols = a_hbm.shape
    quarter, half, strip = rows // 4, rows // 8, rows // 16

    zp, zm = {"kk": (z + 1) % 4 * 4 + y}, {"kk": (z + 3) % 4 * 4 + y}
    yp, ym = {"kk": z * 4 + (y + 1) % 4}, {"kk": z * 4 + (y + 3) % 4}
    gp, gm = {"g": (p + 1) % 8}, {"g": (p + 7) % 8}
    next_chip, last_chip = {"g": (p + 2) % 8}, {"g": (p + 6) % 8}
    odd = p % 2 == 1
    low = p < 4

    own = pltpu.make_async_copy(a_hbm, full.at[:, pl.ds(0, cols)], lsem)
    own.start()
    own_too = pltpu.make_async_copy(a_strips, fully.at[:, :, :, pl.ds(0, cols)], lsem2)
    pl.when(odd)(own_too.start)
    barrier = pltpu.get_barrier_semaphore()
    for dev in (zp, zm, yp, ym, gp, gm):
        pl.semaphore_signal(barrier, inc=1, device_id=dev, device_id_type=MESH)

    @pl.when(odd)
    def _():
        pl.semaphore_signal(barrier, inc=1, device_id=next_chip, device_id_type=MESH)
        pl.semaphore_signal(barrier, inc=1, device_id=last_chip, device_id_type=MESH)

    pl.semaphore_wait(barrier, 6 + p % 2 * 2)
    own.wait()
    pl.when(odd)(own_too.wait)

    slots = iter(range(ssem.shape[0]))

    def copy(src, dst, dev):
        i = next(slots)
        return pltpu.make_async_remote_copy(
            src_ref=src, dst_ref=dst, send_sem=ssem.at[i], recv_sem=rsem.at[i],
            device_id=dev, device_id_type=MESH)

    def start(*copies):
        for c in copies:
            c.start()

    def arrived(*copies):
        for c in copies:
            c.wait_recv()

    def left(*copies):
        for c in copies:
            c.wait_send()

    def q(d):
        return pl.multiple_of((z + d) % 4 * quarter, quarter)

    def shard(first, size, r):
        return full.at[pl.ds(first, size), pl.ds(r * cols, cols)]

    def zplus(first, size, r):
        return copy(shard(first, size, r), shard(first, size, (r + 3) % 4), zp)

    def zminus(first, size, r):
        return copy(shard(first, size, r), shard(first, size, (r + 1) % 4), zm)

    m1, p1 = [zplus(q(1) + h, half, 0) for h in (0, half)], [zminus(q(3) + h, half, 0) for h in (0, half)]
    m2, p2 = zplus(q(2), half, 0), zminus(q(2) + half, half, 0)
    m3, p3 = zplus(q(1), half, 3), zminus(q(3) + half, half, 1)
    m4, p4 = zplus(q(2) + half, half, 0), zminus(q(2), half, 0)
    m9, p9 = zplus(q(0), quarter, 3), zminus(q(0), quarter, 1)
    m7, p7 = zplus(q(0), quarter, 0), zminus(q(0), quarter, 0)
    m5, p5 = zplus(q(3), quarter, 0), zminus(q(1), quarter, 0)
    m8, p8 = zplus(q(3), half, 3), zminus(q(1) + half, half, 1)

    def piece(j, r, first=0, size=quarter):
        if j == 0:
            return shard(q(0) + first, size, r)
        return chunk.at[j - 1, pl.ds(first, size), pl.ds(r * cols, cols)]

    def leg(src, dst, dev):
        return [copy(piece(src, r), piece(dst, r), dev) for r in range(4)]

    def halves(dst, dev):
        return [[copy(piece(0, r, h, half), piece(dst, r, h, half), dev) for h in (0, half)] for r in range(4)]

    x1, x2, x3 = halves(1, gm), leg(1, 2, gm), leg(2, 3, gm)
    x4 = leg(3, 4, gm)
    ARRIVAL = (0, 3, 1, 2)

    def own_piece(r, h):
        x1[r][h].start()

    def yshard(first, r):
        return fully.at[pl.ds(first, 2), :, :, pl.ds(r * cols, cols)]

    def yplus(first, r):
        return copy(yshard(first, r), yshard(first, (r + 3) % 4), yp)

    def yminus(first, r):
        return copy(yshard(first, r), yshard(first, (r + 1) % 4), ym)

    g1, h1, g2, h2 = yplus(0, 0), yminus(2, 0), yplus(2, 0), yminus(0, 0)
    g3, h3 = yplus(0, 3), yminus(2, 1)

    def ypiece(where, r):
        at = pl.ds(r * cols, cols)
        return fully.at[:, y, :, at] if where < 0 else chunky.at[where, :, :, at]

    y1 = [copy(ypiece(-1, r), ypiece(0, r), next_chip) for r in range(4)]
    y2 = [copy(ypiece(0, r), ypiece(1, r), next_chip) for r in range(4)]

    def forward(got, give, shards=ARRIVAL):
        for r in shards:
            arrived(*(got[r] if isinstance(got[r], list) else (got[r],)))
            give[r].start()

    class Unit:
        def __init__(self, j, d0, n, turned=False):
            step = half if j == 4 else quarter
            c0, width = d0 * step, n * step
            hw = width // 2
            self.j, self.ds, self.step, self.turned = j, range(d0, d0 + n), step, turned
            plus, minus, self.at = (zp, zm, z) if turned else (yp, ym, y)
            self.lo, self.hi, self.whole = pl.ds(c0, hw), pl.ds(c0 + hw, hw), pl.ds(c0, width)
            self.land = pl.ds(c0 // 2, hw)
            self.a = copy(part.at[j, self.strip(2), self.lo], sum1.at[0, j, :, self.land], plus)
            self.b = copy(part.at[j, self.strip(2), self.hi], sum1.at[1, j, :, self.land], minus)
            self.c = copy(part.at[j, self.strip(1), self.whole], sum2.at[0, j, :, self.whole], plus)
            self.d = copy(part.at[j, self.strip(3), self.whole], sum2.at[1, j, :, self.whole], minus)
            if j == 4:
                self.sends = [
                    copy(mine.at[2, :, pl.ds(d * step, step)], theirs.at[2, :, pl.ds(d * step, step)],
                         {"kk": z * 4 + (y + d) % 4 if turned else (z + DELTA[d]) % 4 * 4 + y, "g": (p + 4) % 8})
                    for d in self.ds]
            elif j % 2:
                self.sends = [copy(mine.at[j // 2, :, self.whole], theirs.at[j // 2, :, self.whole], gm)]
            else:
                self.sends = []

        def strip(self, d):
            return pl.ds(pl.multiple_of((self.at + d) % 4 * strip, strip), strip)

        def multiply(self, d, lhs, rhs):
            lhs, rhs = (v.reshape(-1, v.shape[-1]) for v in (lhs, rhs))
            part[self.j, :, pl.ds(d * self.step, rhs.shape[0])] = lax.dot_general(
                lhs, rhs, (((1,), (1,)), ((), ())), preferred_element_type=jnp.float32)

        def begin(self):
            j = self.j
            if self.turned:
                self.begin_turned()
            elif j < 4:
                for d in self.ds:
                    rows_j = full[pl.ds(q(0), quarter), :] if j == 0 else chunk[j - 1]
                    self.multiply(d, rows_j, full[pl.ds(q(DELTA[d]), quarter), :])
            else:
                @pl.when(low)
                def _():
                    for d in self.ds:
                        self.multiply(d, chunk[3], full[pl.ds(q(DELTA[d]), half), :])

                @pl.when(~low)
                def _():
                    for d in self.ds:
                        self.multiply(d, full[pl.ds(q(DELTA[d]), quarter), :], chunk[3, half:])
            start(self.a, self.b)

        def begin_turned(self):
            if self.j == 0:
                for d in self.ds:
                    self.multiply(d, fully[:, y], fully[d])
            else:
                @pl.when(low)
                def _():
                    self.multiply(self.ds[0], chunky[1], fully[self.ds[0] // 2])

                @pl.when(~low)
                def _():
                    for d in self.ds:
                        self.multiply(d, fully[:, (y + d) % 4], chunky[1, 2:])

        def middle(self):
            j = self.j
            self.a.wait_recv()
            part[j, self.strip(1), self.lo] += sum1[0, j, :, self.land]
            self.c.start()
            self.b.wait_recv()
            part[j, self.strip(3), self.hi] += sum1[1, j, :, self.land]
            self.d.start()

        def place(self, value):
            if self.turned:
                out_ref[self.j, :, self.whole] = value
                return
            for i, d in enumerate(self.ds):
                out_ref[self.j, :, pl.ds(q(DELTA[d]), self.step)] = value[:, i * self.step:(i + 1) * self.step]

        def end(self):
            j = self.j
            arrived(self.c, self.d)
            total = part[j, self.strip(0), self.whole] + sum2[0, j, :, self.whole] + sum2[1, j, :, self.whole]
            if j == 4:
                @pl.when(low)
                def _():
                    self.place(total)

                @pl.when(~low)
                def _():
                    mine[2, :, self.whole] = total
                    start(*self.sends)
            elif j % 2:
                mine[j // 2, :, self.whole] = total
                start(*self.sends)
            else:
                self.place(total)

        def receive(self):
            arrived(*self.sends)
            if self.j == 4:
                for d in self.ds:
                    first = pl.multiple_of(q(4 - DELTA[d]) + half, half)
                    out_ref[4, :, pl.ds(first, half)] = theirs[2, :, pl.ds(d * half, half)]
            else:
                self.place(theirs[self.j // 2, :, self.whole])

        def settle(self):
            left(self.a, self.b, self.c, self.d)
            if self.j != 4:
                left(*self.sends)

    u00, u10 = Unit(0, 0, 1), Unit(1, 0, 1)
    u01, u11 = Unit(0, 1, 1), Unit(1, 1, 1)
    u20, u21 = Unit(2, 0, 1), Unit(2, 1, 1)
    u02, u12, u22 = Unit(0, 2, 1), Unit(1, 2, 1), Unit(2, 2, 1)
    u03, u13, u23 = Unit(0, 3, 1), Unit(1, 3, 1), Unit(2, 3, 1)
    u30, u31 = Unit(3, 0, 2), Unit(3, 2, 2)
    u40, u41 = Unit(4, 0, 2), Unit(4, 2, 2)
    v00, v01 = Unit(0, 0, 2, turned=True), Unit(0, 2, 2, turned=True)
    v40, v41 = Unit(4, 0, 2, turned=True), Unit(4, 2, 2, turned=True)
    always = (u10, u11, u20, u21, u12, u22, u13, u23, u30, u31)
    even_only, odd_only = (u00, u01, u02, u03, u40, u41), (v00, v01, v40, v41)

    def receive_turned():
        arrived(*v40.sends, *v41.sends)
        cols_of = [theirs[2, :, pl.ds(pl.multiple_of((y + 4 - i) % 4 * half, half), half)] for i in range(4)]
        out_ref[4, :, pl.ds(2 * quarter, quarter)] = jnp.concatenate([v[:, :strip] for v in cols_of], axis=1)
        out_ref[4, :, pl.ds(3 * quarter, quarter)] = jnp.concatenate([v[:, strip:] for v in cols_of], axis=1)

    def both(*steps):
        for step in steps:
            step()

    rest = (m9, p9, m7, p4, m5, p5)

    def head(is_odd):
        start(m2, p2)
        if not is_odd:
            start(m1[0], p1[0], m1[1], p1[1])
        own_piece(0, 0)
        own_piece(0, 1)
        if is_odd:
            start(g1, h1, g2, h2, y1[0])
        arrived(m2)
        start(m3)
        arrived(p2)
        start(p3)
        if is_odd:
            start(m1[0], p1[0], m1[1], p1[1])
        else:
            start(m4, p7)
        forward(x1, x2, shards=(0,))
        if is_odd:
            arrived(g1)
            start(g3)
            arrived(h1)
            start(h3)
        for h in (0, 1):
            arrived(m1[h])
            own_piece(3, h)
            arrived(p1[h])
            own_piece(1, h)
        if not is_odd:
            start(*rest)
        arrived(m3)
        own_piece(2, 0)
        arrived(p3)
        own_piece(2, 1)

    def even_core():
        head(False)
        u00.begin()
        forward(x1, x2, shards=(3, 1, 2))
        u10.begin()
        arrived(m4, p7)
        start(p8)
        arrived(p9)
        both(u01.begin, u11.begin, u00.middle, u10.middle)
        forward(x2, x3, shards=(0, 3))
        arrived(m9, m7)
        start(m8)
        arrived(p4)
        pl.semaphore_signal(gate, inc=1, device_id=gp, device_id_type=MESH)
        both(u02.begin, u12.begin, u01.middle, u11.middle)
        forward(x2, x3, shards=(1, 2))
        both(u20.begin, u21.begin, u22.begin, u12.middle, u02.middle)
        arrived(m5, p5, m8, p8)
        both(u03.begin, u13.begin, u23.begin, u20.middle, u21.middle, u22.middle)
        arrived(*x3)
        both(u30.begin, u31.begin)
        both(u13.middle, u03.middle, u10.end, u11.end, u00.end, u01.end, u30.middle, u31.middle, u12.end)
        arrived(*x4)
        both(u40.begin, u41.begin, u23.middle)
        both(u13.end, u02.end, u20.end, u21.end, u22.end)
        both(u40.middle, u41.middle)
        both(u30.end, u31.end, u40.end, u41.end, u03.end, u23.end)

    def odd_core():
        head(True)
        forward(x1, x2, shards=(3, 1))
        arrived(g2)
        start(y1[3])
        arrived(h2)
        start(y1[1])
        pl.semaphore_wait(gate, 1)
        start(m4, p7, *rest)
        forward(x1, x2, shards=(2,))
        u10.begin()
        arrived(g3, h3)
        start(y1[2])
        forward(x2, x3, shards=(0, 3))
        u10.middle()
        forward(x2, x3, shards=(1,))
        arrived(m4, p7)
        start(p8)
        arrived(p9)
        u11.begin()
        forward(x2, x3, shards=(2,))
        both(u20.begin, u21.begin)
        forward(y1, y2, shards=(0, 3, 1))
        arrived(m9, m7)
        start(m8)
        arrived(p4)
        both(u12.begin, u22.begin, u11.middle, u20.middle, u21.middle)
        forward(y1, y2, shards=(2,))
        arrived(m5, p5, m8, p8)
        both(u13.begin, u23.begin, v00.begin, v01.begin)
        forward(x3, x4, shards=(0, 3))
        both(u12.middle)
        forward(x3, x4, shards=(1, 2))
        both(u30.begin, u31.begin, u13.middle, v00.middle, v01.middle)
        arrived(*y2)
        both(v40.begin, v41.begin, u10.end, u11.end, u20.end, u21.end, u12.end)
        both(u30.middle, u31.middle, v40.middle, v41.middle, u22.middle, u23.middle)
        both(v00.end, v01.end, v40.end, v41.end, u13.end, u30.end, u31.end, u22.end, u23.end)

    pl.when(~odd)(even_core)
    pl.when(odd)(odd_core)
    both(u10.receive, u11.receive, u12.receive, u13.receive, u30.receive, u31.receive)

    @pl.when(low & ~odd)
    def _():
        both(u40.receive, u41.receive)

    @pl.when(low & odd)
    def _():
        receive_turned()

    @pl.when(~low)
    def _():
        out_ref[4] = jnp.zeros(out_ref.shape[1:], out_ref.dtype)

    left(*m1, *p1, m2, p2, m3, p3, m4, p4, m5, p5, m7, p7, m8, p8, m9, p9, *x2, *x3)
    for r in range(4):
        left(*x1[r])
    for u in always:
        u.settle()

    @pl.when(odd)
    def _():
        left(*x4, *y1, *y2, g1, h1, g2, h2, g3, h3)
        for u in odd_only:
            u.settle()

    @pl.when(~odd)
    def _():
        for u in even_only:
            u.settle()

    @pl.when(~low & odd)
    def _():
        left(*v40.sends, *v41.sends)

    @pl.when(~low & ~odd)
    def _():
        left(*u40.sends, *u41.sends)

def solution(mesh):
    def local_fn(a_blk):
        rows, cols = a_blk.shape
        strip = rows // 16
        out = pl.pallas_call(
            kernel,
            out_shape=jax.ShapeDtypeStruct((5, strip, rows), jnp.float32),
            in_specs=[pl.BlockSpec(memory_space=pltpu.HBM)] * 2,
            out_specs=pl.BlockSpec(memory_space=pltpu.VMEM),
            scratch_shapes=[
                pltpu.VMEM((rows, 4 * cols), jnp.bfloat16),
                pltpu.VMEM((4, 4, strip, 4 * cols), jnp.bfloat16),
                pltpu.VMEM((4, rows // 4, 4 * cols), jnp.bfloat16),
                pltpu.VMEM((2, 4, strip, 4 * cols), jnp.bfloat16),
                pltpu.VMEM((5, rows // 4, rows), jnp.float32),
                pltpu.VMEM((2, 5, strip, rows // 2), jnp.float32),
                pltpu.VMEM((2, 5, strip, rows), jnp.float32),
                pltpu.VMEM((3, strip, rows), jnp.float32),
                pltpu.VMEM((3, strip, rows), jnp.float32),
                pltpu.SemaphoreType.DMA((220,)),
                pltpu.SemaphoreType.DMA((220,)),
                pltpu.SemaphoreType.DMA,
                pltpu.SemaphoreType.DMA,
                pltpu.SemaphoreType.REGULAR,
            ],
            compiler_params=pltpu.CompilerParams(
                collective_id=0, has_side_effects=True, vmem_limit_bytes=48 * 1024 * 1024),
        )(pltpu.with_memory_space_constraint(a_blk, pltpu.HBM),
          pltpu.with_memory_space_constraint(a_blk.reshape(4, 4, strip, cols), pltpu.HBM))
        return out[None]

    return jax.shard_map(local_fn, mesh=mesh, in_specs=(P(("m", "g"), "kk"),), out_specs=P(("m", "g"), None, "kk", None), check_vma=False)
```

```python
import functools
import jax
import jax.numpy as jnp
from jax import lax
from jax.experimental import pallas as pl
from jax.experimental.pallas import tpu as pltpu
from jax.sharding import PartitionSpec as P

MESH = pl.DeviceIdType.MESH
DELTA = (0, 1, 3, 2)


def kernel(a_hbm, a_strips, out_ref, full, fully, chunk, chunky, spare, part, sum1, sum2, mine, theirs, ssem, rsem, lsem, lsem2, gate):
    kk, p = lax.axis_index("kk"), lax.axis_index("g")
    z, y = kk // 4, kk % 4
    rows, cols = a_hbm.shape
    quarter, half, strip = rows // 4, rows // 8, rows // 16

    zp, zm = {"kk": (z + 1) % 4 * 4 + y}, {"kk": (z + 3) % 4 * 4 + y}
    yp, ym = {"kk": z * 4 + (y + 1) % 4}, {"kk": z * 4 + (y + 3) % 4}
    gp, gm = {"g": (p + 1) % 8}, {"g": (p + 7) % 8}
    next_chip, last_chip = {"g": (p + 2) % 8}, {"g": (p + 6) % 8}
    across, behind = {"g": (p + 3) % 8}, {"g": (p + 5) % 8}
    odd = p % 2 == 1
    low = p < 4
    relays = (p == 1) | (p == 7)

    own = pltpu.make_async_copy(a_hbm, full.at[:, pl.ds(0, cols)], lsem)
    own.start()
    own_too = pltpu.make_async_copy(a_strips, fully.at[:, :, :, pl.ds(0, cols)], lsem2)
    pl.when(odd)(own_too.start)
    barrier = pltpu.get_barrier_semaphore()
    for dev in (zp, zm, yp, ym, gp, gm, next_chip, last_chip):
        pl.semaphore_signal(barrier, inc=1, device_id=dev, device_id_type=MESH)

    @pl.when(odd)
    def _():
        pl.semaphore_signal(barrier, inc=1, device_id=behind, device_id_type=MESH)

    pl.semaphore_wait(barrier, 9 - p % 2)
    own.wait()
    pl.when(odd)(own_too.wait)

    slots = iter(range(ssem.shape[0]))

    def copy(src, dst, dev):
        i = next(slots)
        return pltpu.make_async_remote_copy(
            src_ref=src, dst_ref=dst, send_sem=ssem.at[i], recv_sem=rsem.at[i],
            device_id=dev, device_id_type=MESH)

    def start(*copies):
        for c in copies:
            c.start()

    def arrived(*copies):
        for c in copies:
            c.wait_recv()

    def left(*copies):
        for c in copies:
            c.wait_send()

    def q(d):
        return pl.multiple_of((z + d) % 4 * quarter, quarter)

    def shard(first, size, r):
        return full.at[pl.ds(first, size), pl.ds(r * cols, cols)]

    def zplus(first, size, r):
        return copy(shard(first, size, r), shard(first, size, (r + 3) % 4), zp)

    def zminus(first, size, r):
        return copy(shard(first, size, r), shard(first, size, (r + 1) % 4), zm)

    m1, p1 = [zplus(q(1) + h, half, 0) for h in (0, half)], [zminus(q(3) + h, half, 0) for h in (0, half)]
    m2, p2 = zplus(q(2), half, 0), zminus(q(2) + half, half, 0)
    m3, p3 = zplus(q(1), half, 3), zminus(q(3) + half, half, 1)
    m4, p4 = zplus(q(2) + half, half, 0), zminus(q(2), half, 0)
    m9, p9 = zplus(q(0), quarter, 3), zminus(q(0), quarter, 1)
    m7, p7 = zplus(q(0), quarter, 0), zminus(q(0), quarter, 0)
    m5, p5 = zplus(q(3), quarter, 0), zminus(q(1), quarter, 0)
    m8, p8 = zplus(q(3), half, 3), zminus(q(1) + half, half, 1)

    def piece(j, r, first=0, size=quarter):
        if j == 0:
            return shard(q(0) + first, size, r)
        return chunk.at[j - 1, pl.ds(first, size), pl.ds(r * cols, cols)]

    def leg(src, dst, dev):
        return [copy(piece(src, r), piece(dst, r), dev) for r in range(4)]

    def halves(dst, dev):
        return [[copy(piece(0, r, h, half), piece(dst, r, h, half), dev) for h in (0, half)] for r in range(4)]

    x1, x2, x3 = halves(1, gm), leg(1, 2, gm), leg(2, 3, gm)
    x4 = leg(3, 4, gm)
    w1 = {r: copy(piece(0, r), spare.at[:, pl.ds(i * cols, cols)], next_chip) for i, r in enumerate((0, 3))}
    w2 = {r: copy(spare.at[:, pl.ds(i * cols, cols)], piece(3, r), across) for i, r in enumerate((0, 3))}
    ARRIVAL = (0, 3, 1, 2)

    def own_piece(r, h):
        x1[r][h].start()

    def yshard(first, r):
        return fully.at[pl.ds(first, 2), :, :, pl.ds(r * cols, cols)]

    def yplus(first, r):
        return copy(yshard(first, r), yshard(first, (r + 3) % 4), yp)

    def yminus(first, r):
        return copy(yshard(first, r), yshard(first, (r + 1) % 4), ym)

    g1, h1, g2, h2 = yplus(0, 0), yminus(2, 0), yplus(2, 0), yminus(0, 0)
    g3, h3 = yplus(0, 3), yminus(2, 1)

    def ypiece(where, r):
        at = pl.ds(r * cols, cols)
        return fully.at[:, y, :, at] if where < 0 else chunky.at[where, :, :, at]

    y1 = [copy(ypiece(-1, r), ypiece(0, r), next_chip) for r in range(4)]
    y2 = [copy(ypiece(0, r), ypiece(1, r), next_chip) for r in range(4)]

    def forward(got, give, shards=ARRIVAL):
        for r in shards:
            arrived(*(got[r] if isinstance(got[r], list) else (got[r],)))
            give[r].start()

    class Unit:
        def __init__(self, j, d0, n, turned=False):
            self.split = j == 4 and not turned
            step = half if self.split else quarter
            c0, width = d0 * step, n * step
            hw = width // 2
            self.j, self.ds, self.step, self.turned = j, range(d0, d0 + n), step, turned
            plus, minus, self.at = (zp, zm, z) if turned else (yp, ym, y)
            self.lo, self.hi, self.whole = pl.ds(c0, hw), pl.ds(c0 + hw, hw), pl.ds(c0, width)
            self.land = pl.ds(c0 // 2, hw)
            self.a = copy(part.at[j, self.strip(2), self.lo], sum1.at[0, j, :, self.land], plus)
            self.b = copy(part.at[j, self.strip(2), self.hi], sum1.at[1, j, :, self.land], minus)
            self.c = copy(part.at[j, self.strip(1), self.whole], sum2.at[0, j, :, self.whole], plus)
            self.d = copy(part.at[j, self.strip(3), self.whole], sum2.at[1, j, :, self.whole], minus)
            self.sends = []
            if self.split:
                for d in self.ds:
                    cols_d = pl.ds(d * step, step)
                    dev = {"kk": (z + DELTA[d]) % 4 * 4 + y, "g": (p + 4) % 8}
                    self.sends.append(copy(mine.at[2, :, cols_d], theirs.at[2, :, cols_d], dev))
            elif j % 2:
                self.sends.append(copy(mine.at[j // 2, :, self.whole], theirs.at[j // 2, :, self.whole], gm))

        def strip(self, d):
            return pl.ds(pl.multiple_of((self.at + d) % 4 * strip, strip), strip)

        def multiply(self, d, lhs, rhs):
            lhs, rhs = (v.reshape(-1, v.shape[-1]) for v in (lhs, rhs))
            part[self.j, :, pl.ds(d * self.step, self.step)] = lax.dot_general(
                lhs, rhs, (((1,), (1,)), ((), ())), preferred_element_type=jnp.float32)

        def product(self):
            j = self.j
            if self.split:
                @pl.when(low)
                def _():
                    for d in self.ds:
                        self.multiply(d, chunk[3], full[pl.ds(q(DELTA[d]), half), :])

                @pl.when(~low)
                def _():
                    for d in self.ds:
                        self.multiply(d, full[pl.ds(q(DELTA[d]), quarter), :], chunk[3, half:])
                return
            for d in self.ds:
                if self.turned:
                    self.multiply(d, fully[:, y] if j == 0 else chunky[1], fully[d])
                else:
                    rows_j = full[pl.ds(q(0), quarter), :] if j == 0 else chunk[j - 1]
                    self.multiply(d, rows_j, full[pl.ds(q(DELTA[d]), quarter), :])

        def middle(self):
            j = self.j
            self.a.wait_recv()
            part[j, self.strip(1), self.lo] += sum1[0, j, :, self.land]
            self.c.start()
            self.b.wait_recv()
            part[j, self.strip(3), self.hi] += sum1[1, j, :, self.land]
            self.d.start()

        def place(self, value):
            if self.turned:
                out_ref[self.j, :, self.whole] = value
                return
            for i, d in enumerate(self.ds):
                out_ref[self.j, :, pl.ds(q(DELTA[d]), self.step)] = value[:, i * self.step:(i + 1) * self.step]

        def end(self):
            j = self.j
            arrived(self.c, self.d)
            total = part[j, self.strip(0), self.whole] + sum2[0, j, :, self.whole] + sum2[1, j, :, self.whole]
            if self.split:
                @pl.when(low)
                def _():
                    self.place(total)

                @pl.when(~low)
                def _():
                    mine[2, :, self.whole] = total
                    start(*self.sends)
            elif self.sends:
                mine[j // 2, :, self.whole] = total
                start(*self.sends)
            else:
                self.place(total)

        def receive(self):
            arrived(*self.sends)
            if not self.split:
                self.place(theirs[self.j // 2, :, self.whole])
                return
            for d in self.ds:
                first = pl.multiple_of(q(4 - DELTA[d]) + half, half)
                out_ref[4, :, pl.ds(first, half)] = theirs[2, :, pl.ds(d * half, half)]

        def settle(self):
            left(self.a, self.b, self.c, self.d)
            if not self.split:
                left(*self.sends)

    u00, u10 = Unit(0, 0, 1), Unit(1, 0, 1)
    u01, u11 = Unit(0, 1, 1), Unit(1, 1, 1)
    u20, u21 = Unit(2, 0, 1), Unit(2, 1, 1)
    u02, u12, u22 = Unit(0, 2, 1), Unit(1, 2, 1), Unit(2, 2, 1)
    u03, u13, u23 = Unit(0, 3, 1), Unit(1, 3, 1), Unit(2, 3, 1)
    u30, u31 = Unit(3, 0, 2), Unit(3, 2, 2)
    u40, u41 = Unit(4, 0, 2), Unit(4, 2, 2)
    v00, v01 = Unit(0, 0, 2, turned=True), Unit(0, 2, 2, turned=True)
    v40, v41 = Unit(4, 0, 2, turned=True), Unit(4, 2, 2, turned=True)
    always = (u10, u11, u20, u21, u12, u22, u13, u23, u30, u31)
    even_only, odd_only = (u00, u01, u02, u03, u40, u41), (v00, v01)

    def begin(*units):
        for i in range(0, len(units), 2):
            for u in units[i:i + 2]:
                u.product()
            for u in units[i:i + 2]:
                start(u.a, u.b)

    def both(*steps):
        for step in steps:
            step()

    rest = (m9, p9, m7, p4, m5, p5)

    def head(is_odd):
        start(m2, p2)
        if not is_odd:
            start(m1[0], p1[0], m1[1], p1[1])
        own_piece(0, 0)
        own_piece(0, 1)
        if not is_odd:
            start(w1[0])
        if is_odd:
            start(g1, h1, g2, h2)
            pl.when(~low)(y1[0].start)
        arrived(m2)
        start(m3)
        arrived(p2)
        start(p3)
        if is_odd:
            start(m1[0], p1[0], m1[1], p1[1])
        else:
            start(m4, p7)
        forward(x1, x2, shards=(0,))
        if is_odd:
            arrived(g1)
            start(g3)
            arrived(h1)
            start(h3)
        for h in (0, 1):
            arrived(m1[h])
            own_piece(3, h)
            arrived(p1[h])
            own_piece(1, h)
        if not is_odd:
            start(w1[3])
            start(*rest)
        arrived(m3)
        own_piece(2, 0)
        arrived(p3)
        own_piece(2, 1)

    def even_core():
        head(False)
        begin(u00)
        forward(w1, w2, shards=(0,))
        forward(x1, x2, shards=(3, 1, 2))
        begin(u10)
        arrived(m4, p7)
        start(p8)
        arrived(p9)
        begin(u01, u11)
        both(u00.middle, u10.middle)
        forward(w1, w2, shards=(3,))
        arrived(x2[0], x2[3])
        arrived(m9, m7)
        start(m8)
        arrived(p4)
        pl.semaphore_signal(gate, inc=1, device_id=gp, device_id_type=MESH)
        begin(u02, u12)
        both(u01.middle, u11.middle)
        forward(x2, x3, shards=(1, 2))
        begin(u20, u21, u22)
        both(u12.middle, u02.middle)
        arrived(m5, p5, m8, p8)
        begin(u03, u13, u23)
        both(u20.middle, u21.middle, u22.middle)
        arrived(*x3)
        begin(u30, u31)
        both(u13.middle, u03.middle, u10.end, u11.end, u00.end, u01.end)
        arrived(*x4)
        begin(u40, u41)
        both(u30.middle, u31.middle, u12.end, u02.end)
        both(u40.middle, u41.middle, u23.middle)
        both(u13.end, u40.end, u41.end, u30.end, u31.end, u20.end, u21.end, u22.end, u03.end, u23.end)

    def pass_on(*shards):
        for r in shards:
            arrived(w2[r] if r in w2 else x3[r])
            x4[r].start()

    def odd_core():
        head(True)
        pl.when(relays)(lambda: forward(y1, y2, shards=(0,)))
        forward(x1, x2, shards=(3, 1))
        arrived(g2)
        pl.when(~low)(y1[3].start)
        arrived(h2)
        pl.when(~low)(y1[1].start)
        pl.semaphore_wait(gate, 1)
        start(m4, p7, *rest)
        forward(x1, x2, shards=(2,))
        begin(u10)
        arrived(g3, h3)
        pl.when(~low)(y1[2].start)
        forward(x2, x3, shards=(0, 3))
        u10.middle()
        pl.when(relays)(lambda: forward(y1, y2, shards=(3,)))
        forward(x2, x3, shards=(1,))
        arrived(m4, p7)
        start(p8)
        arrived(p9)
        begin(u11)
        forward(x2, x3, shards=(2,))
        begin(u20, u21)
        pl.when(relays)(lambda: forward(y1, y2, shards=(1, 2)))
        arrived(m9, m7)
        start(m8)
        arrived(p4)
        begin(u12, u22)
        both(u11.middle, u20.middle, u21.middle)
        pass_on(0, 3, 1, 2)
        arrived(m5, p5, m8, p8)
        begin(u13, u23, u30, u31)
        both(u12.middle)
        begin(v00, v01)
        both(u13.middle)

        def last_pair():
            arrived(*y2)
            begin(v40, v41)

        pl.when(low)(last_pair)
        both(u10.end, u11.end, u20.end, u21.end, u12.end, v00.middle, v01.middle)
        both(u30.middle, u31.middle)
        both(u22.middle, u23.middle)
        pl.when(low)(lambda: both(v40.middle, v41.middle))
        both(u13.end, u30.end, u31.end, v00.end, v01.end, u22.end, u23.end)
        pl.when(low)(lambda: both(v40.end, v41.end))

    pl.when(~odd)(even_core)
    pl.when(odd)(odd_core)
    both(u10.receive, u11.receive, u12.receive, u13.receive, u30.receive, u31.receive)

    @pl.when(low & ~odd)
    def _():
        both(u40.receive, u41.receive)

    @pl.when(~low)
    def _():
        out_ref[4] = jnp.zeros(out_ref.shape[1:], out_ref.dtype)

    left(*m1, *p1, m2, p2, m3, p3, m4, p4, m5, p5, m7, p7, m8, p8, m9, p9, *x2, x3[1], x3[2])
    for r in range(4):
        left(*x1[r])
    for u in always:
        u.settle()

    @pl.when(odd)
    def _():
        left(g1, h1, g2, h2, g3, h3, x3[0], x3[3], *x4)
        for u in odd_only:
            u.settle()

    @pl.when(~odd)
    def _():
        left(w1[0], w1[3], w2[0], w2[3])
        for u in even_only:
            u.settle()

    @pl.when(low & odd)
    def _():
        both(v40.settle, v41.settle)

    @pl.when(~low & ~odd)
    def _():
        left(*u40.sends, *u41.sends)

    pl.when(odd & ~low)(lambda: left(*y1))
    pl.when(relays)(lambda: left(*y2))

def solution(mesh):
    def local_fn(a_blk):
        rows, cols = a_blk.shape
        strip = rows // 16
        out = pl.pallas_call(
            kernel,
            out_shape=jax.ShapeDtypeStruct((5, strip, rows), jnp.float32),
            in_specs=[pl.BlockSpec(memory_space=pltpu.HBM)] * 2,
            out_specs=pl.BlockSpec(memory_space=pltpu.VMEM),
            scratch_shapes=[
                pltpu.VMEM((rows, 4 * cols), jnp.bfloat16),
                pltpu.VMEM((4, 4, strip, 4 * cols), jnp.bfloat16),
                pltpu.VMEM((4, rows // 4, 4 * cols), jnp.bfloat16),
                pltpu.VMEM((2, 4, strip, 4 * cols), jnp.bfloat16),
                pltpu.VMEM((rows // 4, 2 * cols), jnp.bfloat16),
                pltpu.VMEM((5, rows // 4, rows), jnp.float32),
                pltpu.VMEM((2, 5, strip, rows // 2), jnp.float32),
                pltpu.VMEM((2, 5, strip, rows), jnp.float32),
                pltpu.VMEM((3, strip, rows), jnp.float32),
                pltpu.VMEM((3, strip, rows), jnp.float32),
                pltpu.SemaphoreType.DMA((220,)),
                pltpu.SemaphoreType.DMA((220,)),
                pltpu.SemaphoreType.DMA,
                pltpu.SemaphoreType.DMA,
                pltpu.SemaphoreType.REGULAR,
            ],
            compiler_params=pltpu.CompilerParams(
                collective_id=0, has_side_effects=True, vmem_limit_bytes=48 * 1024 * 1024),
        )(pltpu.with_memory_space_constraint(a_blk, pltpu.HBM),
          pltpu.with_memory_space_constraint(a_blk.reshape(4, 4, strip, cols), pltpu.HBM))
        return out[None]

    return jax.shard_map(local_fn, mesh=mesh, in_specs=(P(("m", "g"), "kk"),), out_specs=P(("m", "g"), None, "kk", None), check_vma=False)
```

```python
import functools
import jax
import jax.numpy as jnp
from jax import lax
from jax.experimental import pallas as pl
from jax.experimental.pallas import tpu as pltpu
from jax.sharding import PartitionSpec as P

MESH = pl.DeviceIdType.MESH
DELTA = (0, 1, 3, 2)


def kernel(a_hbm, a_strips, out_ref, full, fully, chunk, chunky, spare, part, sum1, sum2, mine, theirs, ssem, rsem, lsem, lsem2, gate):
    kk, p = lax.axis_index("kk"), lax.axis_index("g")
    z, y = kk // 4, kk % 4
    rows, cols = a_hbm.shape
    quarter, half, strip = rows // 4, rows // 8, rows // 16

    zp, zm = {"kk": (z + 1) % 4 * 4 + y}, {"kk": (z + 3) % 4 * 4 + y}
    yp, ym = {"kk": z * 4 + (y + 1) % 4}, {"kk": z * 4 + (y + 3) % 4}
    gp, gm = {"g": (p + 1) % 8}, {"g": (p + 7) % 8}
    next_chip, last_chip = {"g": (p + 2) % 8}, {"g": (p + 6) % 8}
    across, behind = {"g": (p + 3) % 8}, {"g": (p + 5) % 8}
    odd = p % 2 == 1
    low = p < 4
    relays = (p == 1) | (p == 7)

    own = pltpu.make_async_copy(a_hbm, full.at[:, pl.ds(0, cols)], lsem)
    own.start()
    own_too = pltpu.make_async_copy(a_strips, fully.at[:, :, :, pl.ds(0, cols)], lsem2)
    pl.when(odd)(own_too.start)
    barrier = pltpu.get_barrier_semaphore()
    for dev in (zp, zm, yp, ym, gp, gm, next_chip, last_chip):
        pl.semaphore_signal(barrier, inc=1, device_id=dev, device_id_type=MESH)

    @pl.when(odd)
    def _():
        pl.semaphore_signal(barrier, inc=1, device_id=behind, device_id_type=MESH)

    pl.semaphore_wait(barrier, 9 - p % 2)
    own.wait()
    pl.when(odd)(own_too.wait)

    slots = iter(range(ssem.shape[0]))

    def copy(src, dst, dev):
        i = next(slots)
        return pltpu.make_async_remote_copy(
            src_ref=src, dst_ref=dst, send_sem=ssem.at[i], recv_sem=rsem.at[i],
            device_id=dev, device_id_type=MESH)

    def start(*copies):
        for c in copies:
            c.start()

    def arrived(*copies):
        for c in copies:
            c.wait_recv()

    def left(*copies):
        for c in copies:
            c.wait_send()

    def q(d):
        return pl.multiple_of((z + d) % 4 * quarter, quarter)

    def shard(first, size, r):
        return full.at[pl.ds(first, size), pl.ds(r * cols, cols)]

    def zplus(first, size, r):
        return copy(shard(first, size, r), shard(first, size, (r + 3) % 4), zp)

    def zminus(first, size, r):
        return copy(shard(first, size, r), shard(first, size, (r + 1) % 4), zm)

    m1, p1 = [zplus(q(1) + h, half, 0) for h in (0, half)], [zminus(q(3) + h, half, 0) for h in (0, half)]
    m2, p2 = zplus(q(2), half, 0), zminus(q(2) + half, half, 0)
    m3, p3 = zplus(q(1), half, 3), zminus(q(3) + half, half, 1)
    m4, p4 = zplus(q(2) + half, half, 0), zminus(q(2), half, 0)
    m9, p9 = zplus(q(0), quarter, 3), zminus(q(0), quarter, 1)
    m7, p7 = zplus(q(0), quarter, 0), zminus(q(0), quarter, 0)
    m5, p5 = zplus(q(3), quarter, 0), zminus(q(1), quarter, 0)
    m8, p8 = zplus(q(3), half, 3), zminus(q(1) + half, half, 1)

    def piece(j, r, first=0, size=quarter):
        if j == 0:
            return shard(q(0) + first, size, r)
        return chunk.at[j - 1, pl.ds(first, size), pl.ds(r * cols, cols)]

    def leg(src, dst, dev):
        return [copy(piece(src, r), piece(dst, r), dev) for r in range(4)]

    def halves(dst, dev):
        return [[copy(piece(0, r, h, half), piece(dst, r, h, half), dev) for h in (0, half)] for r in range(4)]

    x1, x2, x3 = halves(1, gm), leg(1, 2, gm), leg(2, 3, gm)
    x4 = leg(3, 4, gm)
    w1 = {r: copy(piece(0, r), spare.at[:, pl.ds(i * cols, cols)], next_chip) for i, r in enumerate((0, 3))}
    w2 = {r: copy(spare.at[:, pl.ds(i * cols, cols)], piece(3, r), across) for i, r in enumerate((0, 3))}
    ARRIVAL = (0, 3, 1, 2)

    def own_piece(r, h):
        x1[r][h].start()

    def yshard(first, r):
        return fully.at[pl.ds(first, 2), :, :, pl.ds(r * cols, cols)]

    def yplus(first, r):
        return copy(yshard(first, r), yshard(first, (r + 3) % 4), yp)

    def yminus(first, r):
        return copy(yshard(first, r), yshard(first, (r + 1) % 4), ym)

    g1, h1, g2, h2 = yplus(0, 0), yminus(2, 0), yplus(2, 0), yminus(0, 0)
    g3, h3 = yplus(0, 3), yminus(2, 1)

    def ypiece(where, r):
        at = pl.ds(r * cols, cols)
        return fully.at[:, y, :, at] if where < 0 else chunky.at[where, :, :, at]

    y1 = [copy(ypiece(-1, r), ypiece(0, r), next_chip) for r in range(4)]
    y2 = [copy(ypiece(0, r), ypiece(1, r), next_chip) for r in range(4)]

    def forward(got, give, shards=ARRIVAL):
        for r in shards:
            arrived(*(got[r] if isinstance(got[r], list) else (got[r],)))
            give[r].start()

    class Unit:
        def __init__(self, j, d0, n, turned=False):
            self.split = j == 4 and not turned
            step = half if self.split else quarter
            c0, width = d0 * step, n * step
            hw = width // 2
            self.j, self.ds, self.step, self.turned = j, range(d0, d0 + n), step, turned
            plus, minus, self.at = (zp, zm, z) if turned else (yp, ym, y)
            self.lo, self.hi, self.whole = pl.ds(c0, hw), pl.ds(c0 + hw, hw), pl.ds(c0, width)
            self.land = pl.ds(c0 // 2, hw)
            self.a = copy(part.at[j, self.strip(2), self.lo], sum1.at[0, j, :, self.land], plus)
            self.b = copy(part.at[j, self.strip(2), self.hi], sum1.at[1, j, :, self.land], minus)
            self.c = copy(part.at[j, self.strip(1), self.whole], sum2.at[0, j, :, self.whole], plus)
            self.d = copy(part.at[j, self.strip(3), self.whole], sum2.at[1, j, :, self.whole], minus)
            self.sends = []
            if self.split:
                for d in self.ds:
                    cols_d = pl.ds(d * step, step)
                    dev = {"kk": (z + DELTA[d]) % 4 * 4 + y, "g": (p + 4) % 8}
                    self.sends.append(copy(mine.at[2, :, cols_d], theirs.at[2, :, cols_d], dev))
            elif j % 2:
                self.sends.append(copy(mine.at[j // 2, :, self.whole], theirs.at[j // 2, :, self.whole], gm))

        def strip(self, d):
            return pl.ds(pl.multiple_of((self.at + d) % 4 * strip, strip), strip)

        def multiply(self, d, lhs, rhs):
            lhs, rhs = (v.reshape(-1, v.shape[-1]) for v in (lhs, rhs))
            part[self.j, :, pl.ds(d * self.step, self.step)] = lax.dot_general(
                lhs, rhs, (((1,), (1,)), ((), ())), preferred_element_type=jnp.float32)

        def product(self):
            j = self.j
            if self.split:
                @pl.when(low)
                def _():
                    for d in self.ds:
                        self.multiply(d, chunk[3], full[pl.ds(q(DELTA[d]), half), :])

                @pl.when(~low)
                def _():
                    for d in self.ds:
                        self.multiply(d, full[pl.ds(q(DELTA[d]), quarter), :], chunk[3, half:])
                return
            for d in self.ds:
                if self.turned:
                    self.multiply(d, fully[:, y] if j == 0 else chunky[1], fully[d])
                else:
                    rows_j = full[pl.ds(q(0), quarter), :] if j == 0 else chunk[j - 1]
                    self.multiply(d, rows_j, full[pl.ds(q(DELTA[d]), quarter), :])

        def middle(self):
            j = self.j
            self.a.wait_recv()
            part[j, self.strip(1), self.lo] += sum1[0, j, :, self.land]
            self.c.start()
            self.b.wait_recv()
            part[j, self.strip(3), self.hi] += sum1[1, j, :, self.land]
            self.d.start()

        def place(self, value):
            if self.turned:
                out_ref[self.j, :, self.whole] = value
                return
            for i, d in enumerate(self.ds):
                out_ref[self.j, :, pl.ds(q(DELTA[d]), self.step)] = value[:, i * self.step:(i + 1) * self.step]

        def end(self):
            j = self.j
            arrived(self.c, self.d)
            total = part[j, self.strip(0), self.whole] + sum2[0, j, :, self.whole] + sum2[1, j, :, self.whole]
            if self.split:
                @pl.when(low)
                def _():
                    self.place(total)

                @pl.when(~low)
                def _():
                    mine[2, :, self.whole] = total
                    start(*self.sends)
            elif self.sends:
                mine[j // 2, :, self.whole] = total
                start(*self.sends)
            else:
                self.place(total)

        def receive(self):
            arrived(*self.sends)
            if not self.split:
                self.place(theirs[self.j // 2, :, self.whole])
                return
            for d in self.ds:
                first = pl.multiple_of(q(4 - DELTA[d]) + half, half)
                out_ref[4, :, pl.ds(first, half)] = theirs[2, :, pl.ds(d * half, half)]

        def settle(self):
            left(self.a, self.b, self.c, self.d)
            if not self.split:
                left(*self.sends)

    u00, u10 = Unit(0, 0, 1), Unit(1, 0, 1)
    u01, u11 = Unit(0, 1, 1), Unit(1, 1, 1)
    u20, u21 = Unit(2, 0, 1), Unit(2, 1, 1)
    u02, u12, u22 = Unit(0, 2, 1), Unit(1, 2, 1), Unit(2, 2, 1)
    u03, u13, u23 = Unit(0, 3, 1), Unit(1, 3, 1), Unit(2, 3, 1)
    u30, u31 = Unit(3, 0, 2), Unit(3, 2, 2)
    u40, u41 = Unit(4, 0, 2), Unit(4, 2, 2)
    v00, v01 = Unit(0, 0, 2, turned=True), Unit(0, 2, 2, turned=True)
    v40, v41 = Unit(4, 0, 2, turned=True), Unit(4, 2, 2, turned=True)
    always = (u10, u11, u20, u21, u12, u22, u13, u23, u30, u31)
    even_only, odd_only = (u00, u01, u02, u03, u40, u41), (v00, v01)

    def begin(*units):
        for i in range(0, len(units), 2):
            for u in units[i:i + 2]:
                u.product()
            for u in units[i:i + 2]:
                start(u.a, u.b)

    def both(*steps):
        for step in steps:
            step()

    rest = (m9, p9, m7, p4, m5, p5)

    def head(is_odd):
        start(m2, p2)
        if not is_odd:
            start(m1[0], p1[0], m1[1], p1[1])
        own_piece(0, 0)
        own_piece(0, 1)
        if not is_odd:
            start(w1[0])
        if is_odd:
            start(g1, h1, g2, h2)
            pl.when(~low)(y1[0].start)
        arrived(m2)
        start(m3)
        arrived(p2)
        start(p3)
        if is_odd:
            start(m1[0], p1[0], m1[1], p1[1])
        else:
            start(m4, p7)
        forward(x1, x2, shards=(0,))
        if is_odd:
            arrived(g1)
            start(g3)
            arrived(h1)
            start(h3)
        for h in (0, 1):
            arrived(m1[h])
            own_piece(3, h)
            arrived(p1[h])
            own_piece(1, h)
        if not is_odd:
            start(w1[3])
            start(*rest)
        arrived(m3)
        own_piece(2, 0)
        arrived(p3)
        own_piece(2, 1)

    def even_core():
        head(False)
        begin(u00)
        forward(w1, w2, shards=(0,))
        forward(x1, x2, shards=(3, 1, 2))
        begin(u10)
        arrived(m4, p7)
        start(p8)
        arrived(p9)
        begin(u01, u11)
        u00.middle()
        arrived(m9, m7)
        start(m8)
        arrived(p4)
        pl.semaphore_signal(gate, inc=1, device_id=gp, device_id_type=MESH)
        u10.middle()
        forward(w1, w2, shards=(3,))
        arrived(x2[0], x2[3])
        begin(u02, u12)
        both(u01.middle, u11.middle)
        forward(x2, x3, shards=(1, 2))
        begin(u20, u21, u22)
        both(u12.middle, u02.middle)
        arrived(m5, p5, m8, p8)
        begin(u03, u13, u23)
        both(u20.middle, u21.middle, u22.middle)
        arrived(*x3)
        begin(u30, u31)
        both(u13.middle, u10.end, u11.end, u00.end, u01.end)
        arrived(*x4)
        begin(u40, u41)
        both(u30.middle, u31.middle, u12.end, u02.end)
        both(u40.middle, u41.middle, u03.middle, u23.middle)
        both(u13.end, u20.end, u21.end, u22.end, u30.end, u31.end, u40.end, u41.end, u03.end, u23.end)

    def pass_on(*shards):
        for r in shards:
            arrived(w2[r] if r in w2 else x3[r])
            x4[r].start()

    def odd_core():
        head(True)
        pl.when(relays)(lambda: forward(y1, y2, shards=(0,)))
        forward(x1, x2, shards=(3, 1))
        arrived(g2)
        pl.when(~low)(y1[3].start)
        arrived(h2)
        pl.when(~low)(y1[1].start)
        pl.semaphore_wait(gate, 1)
        start(m4, p7, *rest)
        forward(x1, x2, shards=(2,))
        begin(u10)
        arrived(g3, h3)
        pl.when(~low)(y1[2].start)
        forward(x2, x3, shards=(0, 3))
        u10.middle()
        forward(x2, x3, shards=(1,))
        arrived(m4, p7)
        start(p8)
        arrived(p9)
        begin(u11)
        pl.when(relays)(lambda: forward(y1, y2, shards=(3,)))
        forward(x2, x3, shards=(2,))
        begin(u20, u21)
        pass_on(0, 3)
        arrived(m9, m7)
        start(m8)
        arrived(p4)
        begin(u12, u22)
        both(u11.middle, u20.middle, u21.middle)
        pass_on(1, 2)
        pl.when(relays)(lambda: forward(y1, y2, shards=(1, 2)))
        arrived(m5, p5, m8, p8)
        begin(u13, u23, u30, u31)
        both(u12.middle)
        begin(v00, v01)
        both(u13.middle)

        def last_pair():
            arrived(*y2)
            begin(v40, v41)

        pl.when(low)(last_pair)
        both(u10.end, u11.end, u20.end, u21.end, u12.end, v00.middle, v01.middle)
        both(u30.middle, u31.middle)
        both(u22.middle, u23.middle)
        pl.when(low)(lambda: both(v40.middle, v41.middle))
        both(u13.end, u30.end, u31.end, v00.end, v01.end, u22.end, u23.end)
        pl.when(low)(lambda: both(v40.end, v41.end))

    pl.when(~odd)(even_core)
    pl.when(odd)(odd_core)
    both(u10.receive, u11.receive, u12.receive, u13.receive, u30.receive, u31.receive)

    @pl.when(low & ~odd)
    def _():
        both(u40.receive, u41.receive)

    @pl.when(~low)
    def _():
        out_ref[4] = jnp.zeros(out_ref.shape[1:], out_ref.dtype)

    left(*m1, *p1, m2, p2, m3, p3, m4, p4, m5, p5, m7, p7, m8, p8, m9, p9, *x2, x3[1], x3[2])
    for r in range(4):
        left(*x1[r])
    for u in always:
        u.settle()

    @pl.when(odd)
    def _():
        left(g1, h1, g2, h2, g3, h3, x3[0], x3[3], *x4)
        for u in odd_only:
            u.settle()

    @pl.when(~odd)
    def _():
        left(w1[0], w1[3], w2[0], w2[3])
        for u in even_only:
            u.settle()

    @pl.when(low & odd)
    def _():
        both(v40.settle, v41.settle)

    @pl.when(~low & ~odd)
    def _():
        left(*u40.sends, *u41.sends)

    pl.when(odd & ~low)(lambda: left(*y1))
    pl.when(relays)(lambda: left(*y2))

def solution(mesh):
    def local_fn(a_blk):
        rows, cols = a_blk.shape
        strip = rows // 16
        out = pl.pallas_call(
            kernel,
            out_shape=jax.ShapeDtypeStruct((5, strip, rows), jnp.float32),
            in_specs=[pl.BlockSpec(memory_space=pltpu.HBM)] * 2,
            out_specs=pl.BlockSpec(memory_space=pltpu.VMEM),
            scratch_shapes=[
                pltpu.VMEM((rows, 4 * cols), jnp.bfloat16),
                pltpu.VMEM((4, 4, strip, 4 * cols), jnp.bfloat16),
                pltpu.VMEM((4, rows // 4, 4 * cols), jnp.bfloat16),
                pltpu.VMEM((2, 4, strip, 4 * cols), jnp.bfloat16),
                pltpu.VMEM((rows // 4, 2 * cols), jnp.bfloat16),
                pltpu.VMEM((5, rows // 4, rows), jnp.float32),
                pltpu.VMEM((2, 5, strip, rows // 2), jnp.float32),
                pltpu.VMEM((2, 5, strip, rows), jnp.float32),
                pltpu.VMEM((3, strip, rows), jnp.float32),
                pltpu.VMEM((3, strip, rows), jnp.float32),
                pltpu.SemaphoreType.DMA((220,)),
                pltpu.SemaphoreType.DMA((220,)),
                pltpu.SemaphoreType.DMA,
                pltpu.SemaphoreType.DMA,
                pltpu.SemaphoreType.REGULAR,
            ],
            compiler_params=pltpu.CompilerParams(
                collective_id=0, has_side_effects=True, vmem_limit_bytes=48 * 1024 * 1024),
        )(pltpu.with_memory_space_constraint(a_blk, pltpu.HBM),
          pltpu.with_memory_space_constraint(a_blk.reshape(4, 4, strip, cols), pltpu.HBM))
        return out[None]

    return jax.shard_map(local_fn, mesh=mesh, in_specs=(P(("m", "g"), "kk"),), out_specs=P(("m", "g"), None, "kk", None), check_vma=False)
```

```python
import functools
import jax
import jax.numpy as jnp
from jax import lax
from jax.experimental import pallas as pl
from jax.experimental.pallas import tpu as pltpu
from jax.sharding import PartitionSpec as P

MESH = pl.DeviceIdType.MESH
DELTA = (0, 1, 3, 2)


def kernel(a_hbm, a_strips, out_ref, full, fully, chunk, chunky, spare, part, sum1, sum2, mine, theirs, ssem, rsem, lsem, lsem2, gate):
    kk, p = lax.axis_index("kk"), lax.axis_index("g")
    z, y = kk // 4, kk % 4
    rows, cols = a_hbm.shape
    quarter, half, strip = rows // 4, rows // 8, rows // 16

    zp, zm = {"kk": (z + 1) % 4 * 4 + y}, {"kk": (z + 3) % 4 * 4 + y}
    yp, ym = {"kk": z * 4 + (y + 1) % 4}, {"kk": z * 4 + (y + 3) % 4}
    gp, gm = {"g": (p + 1) % 8}, {"g": (p + 7) % 8}
    next_chip, last_chip = {"g": (p + 2) % 8}, {"g": (p + 6) % 8}
    across, behind = {"g": (p + 3) % 8}, {"g": (p + 5) % 8}
    odd = p % 2 == 1
    low = p < 4
    relays = (p == 1) | (p == 7)

    own = pltpu.make_async_copy(a_hbm, full.at[:, pl.ds(0, cols)], lsem)
    own.start()
    own_too = pltpu.make_async_copy(a_strips, fully.at[:, :, :, pl.ds(0, cols)], lsem2)
    pl.when(odd)(own_too.start)
    barrier = pltpu.get_barrier_semaphore()
    for dev in (zp, zm, yp, ym, gp, gm, next_chip, last_chip):
        pl.semaphore_signal(barrier, inc=1, device_id=dev, device_id_type=MESH)

    @pl.when(odd)
    def _():
        pl.semaphore_signal(barrier, inc=1, device_id=behind, device_id_type=MESH)

    pl.semaphore_wait(barrier, 9 - p % 2)
    own.wait()
    pl.when(odd)(own_too.wait)

    slots = iter(range(ssem.shape[0]))

    def copy(src, dst, dev):
        i = next(slots)
        return pltpu.make_async_remote_copy(
            src_ref=src, dst_ref=dst, send_sem=ssem.at[i], recv_sem=rsem.at[i],
            device_id=dev, device_id_type=MESH)

    def start(*copies):
        for c in copies:
            c.start()

    def arrived(*copies):
        for c in copies:
            c.wait_recv()

    def left(*copies):
        for c in copies:
            c.wait_send()

    def q(d):
        return pl.multiple_of((z + d) % 4 * quarter, quarter)

    def shard(first, size, r):
        return full.at[pl.ds(first, size), pl.ds(r * cols, cols)]

    def zplus(first, size, r):
        return copy(shard(first, size, r), shard(first, size, (r + 3) % 4), zp)

    def zminus(first, size, r):
        return copy(shard(first, size, r), shard(first, size, (r + 1) % 4), zm)

    m1, p1 = [zplus(q(1) + h, half, 0) for h in (0, half)], [zminus(q(3) + h, half, 0) for h in (0, half)]
    m2, p2 = zplus(q(2), half, 0), zminus(q(2) + half, half, 0)
    m3, p3 = zplus(q(1), half, 3), zminus(q(3) + half, half, 1)
    m4, p4 = zplus(q(2) + half, half, 0), zminus(q(2), half, 0)
    m9, p9 = zplus(q(0), quarter, 3), zminus(q(0), quarter, 1)
    m7, p7 = zplus(q(0), quarter, 0), zminus(q(0), quarter, 0)
    m5, p5 = zplus(q(3), quarter, 0), zminus(q(1), quarter, 0)
    m8, p8 = zplus(q(3), half, 3), zminus(q(1) + half, half, 1)

    def piece(j, r, first=0, size=quarter):
        if j == 0:
            return shard(q(0) + first, size, r)
        return chunk.at[j - 1, pl.ds(first, size), pl.ds(r * cols, cols)]

    def leg(src, dst, dev):
        return [copy(piece(src, r), piece(dst, r), dev) for r in range(4)]

    def halves(dst, dev):
        return [[copy(piece(0, r, h, half), piece(dst, r, h, half), dev) for h in (0, half)] for r in range(4)]

    x1, x2, x3 = halves(1, gm), leg(1, 2, gm), leg(2, 3, gm)
    x4 = leg(3, 4, gm)
    w1 = {r: copy(piece(0, r), spare.at[:, pl.ds(i * cols, cols)], next_chip) for i, r in enumerate((0, 3))}
    w2 = {r: copy(spare.at[:, pl.ds(i * cols, cols)], piece(3, r), across) for i, r in enumerate((0, 3))}
    ARRIVAL = (0, 3, 1, 2)

    def own_piece(r, h):
        x1[r][h].start()

    def yshard(first, r):
        return fully.at[pl.ds(first, 2), :, :, pl.ds(r * cols, cols)]

    def yplus(first, r):
        return copy(yshard(first, r), yshard(first, (r + 3) % 4), yp)

    def yminus(first, r):
        return copy(yshard(first, r), yshard(first, (r + 1) % 4), ym)

    g1, h1, g2, h2 = yplus(0, 0), yminus(2, 0), yplus(2, 0), yminus(0, 0)
    g3, h3 = yplus(0, 3), yminus(2, 1)

    def ypiece(where, r):
        at = pl.ds(r * cols, cols)
        return fully.at[:, y, :, at] if where < 0 else chunky.at[where, :, :, at]

    y1 = [copy(ypiece(-1, r), ypiece(0, r), next_chip) for r in range(4)]
    y2 = [copy(ypiece(0, r), ypiece(1, r), next_chip) for r in range(4)]

    def forward(got, give, shards=ARRIVAL):
        for r in shards:
            arrived(*(got[r] if isinstance(got[r], list) else (got[r],)))
            give[r].start()

    class Unit:
        def __init__(self, j, d0, n, turned=False):
            self.split = j == 4 and not turned
            step = half if self.split else quarter
            c0, width = d0 * step, n * step
            hw = width // 2
            self.j, self.ds, self.step, self.turned = j, range(d0, d0 + n), step, turned
            plus, minus, self.at = (zp, zm, z) if turned else (yp, ym, y)
            self.lo, self.hi, self.whole = pl.ds(c0, hw), pl.ds(c0 + hw, hw), pl.ds(c0, width)
            self.land = pl.ds(c0 // 2, hw)
            self.a = copy(part.at[j, self.strip(2), self.lo], sum1.at[0, j, :, self.land], plus)
            self.b = copy(part.at[j, self.strip(2), self.hi], sum1.at[1, j, :, self.land], minus)
            self.c = copy(part.at[j, self.strip(1), self.whole], sum2.at[0, j, :, self.whole], plus)
            self.d = copy(part.at[j, self.strip(3), self.whole], sum2.at[1, j, :, self.whole], minus)
            self.sends = []
            if self.split:
                for d in self.ds:
                    cols_d = pl.ds(d * step, step)
                    dev = {"kk": (z + DELTA[d]) % 4 * 4 + y, "g": (p + 4) % 8}
                    self.sends.append(copy(mine.at[2, :, cols_d], theirs.at[2, :, cols_d], dev))
            elif j % 2:
                self.sends.append(copy(mine.at[j // 2, :, self.whole], theirs.at[j // 2, :, self.whole], gm))

        def strip(self, d):
            return pl.ds(pl.multiple_of((self.at + d) % 4 * strip, strip), strip)

        def multiply(self, d, lhs, rhs):
            lhs, rhs = (v.reshape(-1, v.shape[-1]) for v in (lhs, rhs))
            part[self.j, :, pl.ds(d * self.step, self.step)] = lax.dot_general(
                lhs, rhs, (((1,), (1,)), ((), ())), preferred_element_type=jnp.float32)

        def product(self):
            j = self.j
            if self.split:
                @pl.when(low)
                def _():
                    for d in self.ds:
                        self.multiply(d, chunk[3], full[pl.ds(q(DELTA[d]), half), :])

                @pl.when(~low)
                def _():
                    for d in self.ds:
                        self.multiply(d, full[pl.ds(q(DELTA[d]), quarter), :], chunk[3, half:])
                return
            for d in self.ds:
                if self.turned:
                    self.multiply(d, fully[:, y] if j == 0 else chunky[1], fully[d])
                else:
                    rows_j = full[pl.ds(q(0), quarter), :] if j == 0 else chunk[j - 1]
                    self.multiply(d, rows_j, full[pl.ds(q(DELTA[d]), quarter), :])

        def middle(self):
            j = self.j
            self.a.wait_recv()
            part[j, self.strip(1), self.lo] += sum1[0, j, :, self.land]
            self.c.start()
            self.b.wait_recv()
            part[j, self.strip(3), self.hi] += sum1[1, j, :, self.land]
            self.d.start()

        def place(self, value):
            if self.turned:
                out_ref[self.j, :, self.whole] = value
                return
            for i, d in enumerate(self.ds):
                out_ref[self.j, :, pl.ds(q(DELTA[d]), self.step)] = value[:, i * self.step:(i + 1) * self.step]

        def end(self):
            j = self.j
            arrived(self.c, self.d)
            total = part[j, self.strip(0), self.whole] + sum2[0, j, :, self.whole] + sum2[1, j, :, self.whole]
            if self.split:
                @pl.when(low)
                def _():
                    self.place(total)

                @pl.when(~low)
                def _():
                    mine[2, :, self.whole] = total
                    start(*self.sends)
            elif self.sends:
                mine[j // 2, :, self.whole] = total
                start(*self.sends)
            else:
                self.place(total)

        def receive(self):
            arrived(*self.sends)
            if not self.split:
                self.place(theirs[self.j // 2, :, self.whole])
                return
            for d in self.ds:
                first = pl.multiple_of(q(4 - DELTA[d]) + half, half)
                out_ref[4, :, pl.ds(first, half)] = theirs[2, :, pl.ds(d * half, half)]

        def settle(self):
            left(self.a, self.b, self.c, self.d)
            if not self.split:
                left(*self.sends)

    u00, u10 = Unit(0, 0, 1), Unit(1, 0, 1)
    u01, u11 = Unit(0, 1, 1), Unit(1, 1, 1)
    u20, u21 = Unit(2, 0, 1), Unit(2, 1, 1)
    u02, u12, u22 = Unit(0, 2, 1), Unit(1, 2, 1), Unit(2, 2, 1)
    u03, u13, u23 = Unit(0, 3, 1), Unit(1, 3, 1), Unit(2, 3, 1)
    u30, u31 = Unit(3, 0, 2), Unit(3, 2, 2)
    u40, u41 = Unit(4, 0, 2), Unit(4, 2, 2)
    v00, v01 = Unit(0, 0, 2, turned=True), Unit(0, 2, 2, turned=True)
    v40, v41 = Unit(4, 0, 2, turned=True), Unit(4, 2, 2, turned=True)
    always = (u10, u11, u20, u21, u12, u22, u13, u23, u30, u31)
    even_only, odd_only = (u00, u01, u02, u03, u40, u41), (v00, v01)

    def begin(*units):
        for i in range(0, len(units), 2):
            for u in units[i:i + 2]:
                u.product()
            for u in units[i:i + 2]:
                start(u.a, u.b)

    def both(*steps):
        for step in steps:
            step()

    rest = (m9, p9, m7, p4, m5, p5)

    def head(is_odd):
        start(m2, p2)
        if not is_odd:
            start(m1[0], p1[0], m1[1], p1[1])
        own_piece(0, 0)
        own_piece(0, 1)
        if not is_odd:
            start(w1[0])
        if is_odd:
            start(g1, h1, g2, h2)
            pl.when(~low)(y1[0].start)
        arrived(m2)
        start(m3)
        arrived(p2)
        start(p3)
        if is_odd:
            start(m1[0], p1[0], m1[1], p1[1])
        else:
            start(m4, p7)
        forward(x1, x2, shards=(0,))
        if is_odd:
            arrived(g1)
            start(g3)
            arrived(h1)
            start(h3)
        for h in (0, 1):
            arrived(m1[h])
            own_piece(3, h)
            arrived(p1[h])
            own_piece(1, h)
        if not is_odd:
            start(w1[3])
            start(*rest)
        arrived(m3)
        own_piece(2, 0)
        arrived(p3)
        own_piece(2, 1)

    def even_core():
        head(False)
        begin(u00)
        forward(w1, w2, shards=(0,))
        forward(x1, x2, shards=(3, 1, 2))
        begin(u10)
        arrived(m4, p7)
        start(p8)
        arrived(p9)
        begin(u01, u11)
        u00.middle()
        arrived(m9, m7)
        start(m8)
        arrived(p4)
        pl.semaphore_signal(gate, inc=1, device_id=gp, device_id_type=MESH)
        u10.middle()
        forward(w1, w2, shards=(3,))
        arrived(x2[0], x2[3])
        begin(u02, u12)
        both(u01.middle, u11.middle)
        forward(x2, x3, shards=(1, 2))
        begin(u20, u21, u22)
        both(u12.middle, u02.middle)
        arrived(m5, p5, m8, p8)
        begin(u03, u13, u23)
        both(u20.middle, u21.middle, u22.middle)
        arrived(*x3)
        begin(u30, u31)
        both(u13.middle, u10.end, u11.end, u00.end, u01.end)
        arrived(*x4)
        begin(u40, u41)
        both(u30.middle, u12.end, u02.end)
        both(u40.middle, u41.middle, u31.middle, u03.middle, u23.middle)
        both(u13.end, u20.end, u21.end, u22.end, u30.end, u40.end, u41.end, u31.end, u03.end, u23.end)

    def pass_on(*shards):
        for r in shards:
            arrived(w2[r] if r in w2 else x3[r])
            x4[r].start()

    def odd_core():
        head(True)
        pl.when(relays)(lambda: forward(y1, y2, shards=(0,)))
        forward(x1, x2, shards=(3, 1))
        arrived(g2)
        pl.when(~low)(y1[3].start)
        arrived(h2)
        pl.when(~low)(y1[1].start)
        pl.semaphore_wait(gate, 1)
        start(m4, p7, *rest)
        forward(x1, x2, shards=(2,))
        begin(u10)
        arrived(g3, h3)
        pl.when(~low)(y1[2].start)
        forward(x2, x3, shards=(0, 3))
        u10.middle()
        forward(x2, x3, shards=(1,))
        arrived(m4, p7)
        start(p8)
        arrived(p9)
        begin(u11)
        pl.when(relays)(lambda: forward(y1, y2, shards=(3,)))
        forward(x2, x3, shards=(2,))
        begin(u20, u21)
        pass_on(0, 3)
        arrived(m9, m7)
        start(m8)
        arrived(p4)
        begin(u12, u22)
        pl.when(relays)(lambda: forward(y1, y2, shards=(1,)))
        both(u11.middle, u20.middle, u21.middle)
        pass_on(1, 2)
        pl.when(relays)(lambda: forward(y1, y2, shards=(2,)))
        arrived(m5, p5, m8, p8)
        begin(u13, u23, u30, u31)
        both(u12.middle)
        begin(v00, v01)

        def last_pair():
            arrived(*y2)
            begin(v40, v41)

        pl.when(low)(last_pair)
        both(u13.middle)
        both(u10.end, u11.end, u20.end, u21.end, v00.middle, v01.middle)
        both(u30.middle, u31.middle, u12.end)
        both(u22.middle, u23.middle)
        pl.when(low)(lambda: both(v40.middle, v41.middle))
        both(u13.end, u30.end, u31.end, v00.end, v01.end, u22.end, u23.end)
        pl.when(low)(lambda: both(v40.end, v41.end))

    pl.when(~odd)(even_core)
    pl.when(odd)(odd_core)
    both(u10.receive, u11.receive, u12.receive, u13.receive, u30.receive, u31.receive)

    @pl.when(low & ~odd)
    def _():
        both(u40.receive, u41.receive)

    @pl.when(~low)
    def _():
        out_ref[4] = jnp.zeros(out_ref.shape[1:], out_ref.dtype)

    left(*m1, *p1, m2, p2, m3, p3, m4, p4, m5, p5, m7, p7, m8, p8, m9, p9, *x2, x3[1], x3[2])
    for r in range(4):
        left(*x1[r])
    for u in always:
        u.settle()

    @pl.when(odd)
    def _():
        left(g1, h1, g2, h2, g3, h3, x3[0], x3[3], *x4)
        for u in odd_only:
            u.settle()

    @pl.when(~odd)
    def _():
        left(w1[0], w1[3], w2[0], w2[3])
        for u in even_only:
            u.settle()

    @pl.when(low & odd)
    def _():
        both(v40.settle, v41.settle)

    @pl.when(~low & ~odd)
    def _():
        left(*u40.sends, *u41.sends)

    pl.when(odd & ~low)(lambda: left(*y1))
    pl.when(relays)(lambda: left(*y2))

def solution(mesh):
    def local_fn(a_blk):
        rows, cols = a_blk.shape
        strip = rows // 16
        out = pl.pallas_call(
            kernel,
            out_shape=jax.ShapeDtypeStruct((5, strip, rows), jnp.float32),
            in_specs=[pl.BlockSpec(memory_space=pltpu.HBM)] * 2,
            out_specs=pl.BlockSpec(memory_space=pltpu.VMEM),
            scratch_shapes=[
                pltpu.VMEM((rows, 4 * cols), jnp.bfloat16),
                pltpu.VMEM((4, 4, strip, 4 * cols), jnp.bfloat16),
                pltpu.VMEM((4, rows // 4, 4 * cols), jnp.bfloat16),
                pltpu.VMEM((2, 4, strip, 4 * cols), jnp.bfloat16),
                pltpu.VMEM((rows // 4, 2 * cols), jnp.bfloat16),
                pltpu.VMEM((5, rows // 4, rows), jnp.float32),
                pltpu.VMEM((2, 5, strip, rows // 2), jnp.float32),
                pltpu.VMEM((2, 5, strip, rows), jnp.float32),
                pltpu.VMEM((3, strip, rows), jnp.float32),
                pltpu.VMEM((3, strip, rows), jnp.float32),
                pltpu.SemaphoreType.DMA((220,)),
                pltpu.SemaphoreType.DMA((220,)),
                pltpu.SemaphoreType.DMA,
                pltpu.SemaphoreType.DMA,
                pltpu.SemaphoreType.REGULAR,
            ],
            compiler_params=pltpu.CompilerParams(
                collective_id=0, has_side_effects=True, vmem_limit_bytes=48 * 1024 * 1024),
        )(pltpu.with_memory_space_constraint(a_blk, pltpu.HBM),
          pltpu.with_memory_space_constraint(a_blk.reshape(4, 4, strip, cols), pltpu.HBM))
        return out[None]

    return jax.shard_map(local_fn, mesh=mesh, in_specs=(P(("m", "g"), "kk"),), out_specs=P(("m", "g"), None, "kk", None), check_vma=False)
```

```python
import functools
import jax
import jax.numpy as jnp
from jax import lax
from jax.experimental import pallas as pl
from jax.experimental.pallas import tpu as pltpu
from jax.sharding import PartitionSpec as P

MESH = pl.DeviceIdType.MESH
DELTA = (0, 1, 3, 2)


def kernel(a_hbm, a_strips, out_ref, full, fully, chunk, chunky, spare, part, sum1, sum2, mine, theirs, ssem, rsem, lsem, lsem2, gate):
    kk, p = lax.axis_index("kk"), lax.axis_index("g")
    z, y = kk // 4, kk % 4
    rows, cols = a_hbm.shape
    quarter, half, strip = rows // 4, rows // 8, rows // 16

    zp, zm = {"kk": (z + 1) % 4 * 4 + y}, {"kk": (z + 3) % 4 * 4 + y}
    yp, ym = {"kk": z * 4 + (y + 1) % 4}, {"kk": z * 4 + (y + 3) % 4}
    gp, gm = {"g": (p + 1) % 8}, {"g": (p + 7) % 8}
    next_chip, last_chip = {"g": (p + 2) % 8}, {"g": (p + 6) % 8}
    across, behind = {"g": (p + 3) % 8}, {"g": (p + 5) % 8}
    odd = p % 2 == 1
    low = p < 4
    relays = (p == 1) | (p == 7)

    own = pltpu.make_async_copy(a_hbm, full.at[:, pl.ds(0, cols)], lsem)
    own.start()
    own_too = pltpu.make_async_copy(a_strips, fully.at[:, :, :, pl.ds(0, cols)], lsem2)
    pl.when(odd)(own_too.start)
    barrier = pltpu.get_barrier_semaphore()
    for dev in (zp, zm, yp, ym, gp, gm, next_chip, last_chip):
        pl.semaphore_signal(barrier, inc=1, device_id=dev, device_id_type=MESH)

    @pl.when(odd)
    def _():
        pl.semaphore_signal(barrier, inc=1, device_id=behind, device_id_type=MESH)

    pl.semaphore_wait(barrier, 9 - p % 2)
    own.wait()
    pl.when(odd)(own_too.wait)

    slots = iter(range(ssem.shape[0]))

    def copy(src, dst, dev):
        i = next(slots)
        return pltpu.make_async_remote_copy(
            src_ref=src, dst_ref=dst, send_sem=ssem.at[i], recv_sem=rsem.at[i],
            device_id=dev, device_id_type=MESH)

    def start(*copies):
        for c in copies:
            c.start()

    def arrived(*copies):
        for c in copies:
            c.wait_recv()

    def left(*copies):
        for c in copies:
            c.wait_send()

    def q(d):
        return pl.multiple_of((z + d) % 4 * quarter, quarter)

    def shard(first, size, r):
        return full.at[pl.ds(first, size), pl.ds(r * cols, cols)]

    def zplus(first, size, r):
        return copy(shard(first, size, r), shard(first, size, (r + 3) % 4), zp)

    def zminus(first, size, r):
        return copy(shard(first, size, r), shard(first, size, (r + 1) % 4), zm)

    m1, p1 = [zplus(q(1) + h, half, 0) for h in (0, half)], [zminus(q(3) + h, half, 0) for h in (0, half)]
    m2, p2 = zplus(q(2), half, 0), zminus(q(2) + half, half, 0)
    m3, p3 = zplus(q(1), half, 3), zminus(q(3) + half, half, 1)
    m4, p4 = zplus(q(2) + half, half, 0), zminus(q(2), half, 0)
    m9, p9 = zplus(q(0), quarter, 3), zminus(q(0), quarter, 1)
    m7, p7 = zplus(q(0), quarter, 0), zminus(q(0), quarter, 0)
    m5, p5 = zplus(q(3), quarter, 0), zminus(q(1), quarter, 0)
    m8, p8 = zplus(q(3), half, 3), zminus(q(1) + half, half, 1)

    def piece(j, r, first=0, size=quarter):
        if j == 0:
            return shard(q(0) + first, size, r)
        return chunk.at[j - 1, pl.ds(first, size), pl.ds(r * cols, cols)]

    def leg(src, dst, dev):
        return [copy(piece(src, r), piece(dst, r), dev) for r in range(4)]

    def halves(dst, dev):
        return [[copy(piece(0, r, h, half), piece(dst, r, h, half), dev) for h in (0, half)] for r in range(4)]

    x1, x2, x3 = halves(1, gm), leg(1, 2, gm), leg(2, 3, gm)
    x4 = leg(3, 4, gm)
    w1 = {r: copy(piece(0, r), spare.at[:, pl.ds(i * cols, cols)], next_chip) for i, r in enumerate((0, 3))}
    w2 = {r: copy(spare.at[:, pl.ds(i * cols, cols)], piece(3, r), across) for i, r in enumerate((0, 3))}
    ARRIVAL = (0, 3, 1, 2)

    def own_piece(r, h):
        x1[r][h].start()

    def yshard(first, r):
        return fully.at[pl.ds(first, 2), :, :, pl.ds(r * cols, cols)]

    def yplus(first, r):
        return copy(yshard(first, r), yshard(first, (r + 3) % 4), yp)

    def yminus(first, r):
        return copy(yshard(first, r), yshard(first, (r + 1) % 4), ym)

    g1, h1, g2, h2 = yplus(0, 0), yminus(2, 0), yplus(2, 0), yminus(0, 0)
    g3, h3 = yplus(0, 3), yminus(2, 1)

    def ypiece(where, r):
        at = pl.ds(r * cols, cols)
        return fully.at[:, y, :, at] if where < 0 else chunky.at[where, :, :, at]

    y1 = [copy(ypiece(-1, r), ypiece(0, r), next_chip) for r in range(4)]
    y2 = [copy(ypiece(0, r), ypiece(1, r), next_chip) for r in range(4)]

    def forward(got, give, shards=ARRIVAL):
        for r in shards:
            arrived(*(got[r] if isinstance(got[r], list) else (got[r],)))
            give[r].start()

    class Unit:
        def __init__(self, j, d0, n, turned=False):
            self.split = j == 4 and not turned
            step = half if self.split else quarter
            c0, width = d0 * step, n * step
            hw = width // 2
            self.j, self.ds, self.step, self.turned = j, range(d0, d0 + n), step, turned
            plus, minus, self.at = (zp, zm, z) if turned else (yp, ym, y)
            self.lo, self.hi, self.whole = pl.ds(c0, hw), pl.ds(c0 + hw, hw), pl.ds(c0, width)
            self.land = pl.ds(c0 // 2, hw)
            self.a = copy(part.at[j, self.strip(2), self.lo], sum1.at[0, j, :, self.land], plus)
            self.b = copy(part.at[j, self.strip(2), self.hi], sum1.at[1, j, :, self.land], minus)
            self.c = copy(part.at[j, self.strip(1), self.whole], sum2.at[0, j, :, self.whole], plus)
            self.d = copy(part.at[j, self.strip(3), self.whole], sum2.at[1, j, :, self.whole], minus)
            self.sends = []
            if self.split:
                for d in self.ds:
                    cols_d = pl.ds(d * step, step)
                    dev = {"kk": (z + DELTA[d]) % 4 * 4 + y, "g": (p + 4) % 8}
                    self.sends.append(copy(mine.at[2, :, cols_d], theirs.at[2, :, cols_d], dev))
            elif j % 2:
                self.sends.append(copy(mine.at[j // 2, :, self.whole], theirs.at[j // 2, :, self.whole], gm))

        def strip(self, d):
            return pl.ds(pl.multiple_of((self.at + d) % 4 * strip, strip), strip)

        def multiply(self, d, lhs, rhs):
            lhs, rhs = (v.reshape(-1, v.shape[-1]) for v in (lhs, rhs))
            part[self.j, :, pl.ds(d * self.step, self.step)] = lax.dot_general(
                lhs, rhs, (((1,), (1,)), ((), ())), preferred_element_type=jnp.float32)

        def product(self):
            j = self.j
            if self.split:
                @pl.when(low)
                def _():
                    for d in self.ds:
                        self.multiply(d, chunk[3], full[pl.ds(q(DELTA[d]), half), :])

                @pl.when(~low)
                def _():
                    for d in self.ds:
                        self.multiply(d, full[pl.ds(q(DELTA[d]), quarter), :], chunk[3, half:])
                return
            for d in self.ds:
                if self.turned:
                    self.multiply(d, fully[:, y] if j == 0 else chunky[1], fully[d])
                else:
                    rows_j = full[pl.ds(q(0), quarter), :] if j == 0 else chunk[j - 1]
                    self.multiply(d, rows_j, full[pl.ds(q(DELTA[d]), quarter), :])

        def middle(self):
            j = self.j
            self.a.wait_recv()
            part[j, self.strip(1), self.lo] += sum1[0, j, :, self.land]
            self.c.start()
            self.b.wait_recv()
            part[j, self.strip(3), self.hi] += sum1[1, j, :, self.land]
            self.d.start()

        def place(self, value):
            if self.turned:
                out_ref[self.j, :, self.whole] = value
                return
            for i, d in enumerate(self.ds):
                out_ref[self.j, :, pl.ds(q(DELTA[d]), self.step)] = value[:, i * self.step:(i + 1) * self.step]

        def end(self):
            j = self.j
            arrived(self.c, self.d)
            total = part[j, self.strip(0), self.whole] + sum2[0, j, :, self.whole] + sum2[1, j, :, self.whole]
            if self.split:
                @pl.when(low)
                def _():
                    self.place(total)

                @pl.when(~low)
                def _():
                    mine[2, :, self.whole] = total
                    start(*self.sends)
            elif self.sends:
                mine[j // 2, :, self.whole] = total
                start(*self.sends)
            else:
                self.place(total)

        def receive(self):
            arrived(*self.sends)
            if not self.split:
                self.place(theirs[self.j // 2, :, self.whole])
                return
            for d in self.ds:
                first = pl.multiple_of(q(4 - DELTA[d]) + half, half)
                out_ref[4, :, pl.ds(first, half)] = theirs[2, :, pl.ds(d * half, half)]

        def settle(self):
            left(self.a, self.b, self.c, self.d)
            if not self.split:
                left(*self.sends)

    u00, u10 = Unit(0, 0, 1), Unit(1, 0, 1)
    u01, u11 = Unit(0, 1, 1), Unit(1, 1, 1)
    u20, u21 = Unit(2, 0, 1), Unit(2, 1, 1)
    u02, u12, u22 = Unit(0, 2, 1), Unit(1, 2, 1), Unit(2, 2, 1)
    u03, u13, u23 = Unit(0, 3, 1), Unit(1, 3, 1), Unit(2, 3, 1)
    u30, u31 = Unit(3, 0, 2), Unit(3, 2, 2)
    u40, u41 = Unit(4, 0, 2), Unit(4, 2, 2)
    v00, v01 = Unit(0, 0, 2, turned=True), Unit(0, 2, 2, turned=True)
    v40, v41 = Unit(4, 0, 2, turned=True), Unit(4, 2, 2, turned=True)
    always = (u10, u11, u20, u21, u12, u22, u13, u23, u30, u31)
    even_only, odd_only = (u00, u01, u02, u03, u40, u41), (v00, v01)

    def begin(*units):
        for i in range(0, len(units), 2):
            for u in units[i:i + 2]:
                u.product()
            for u in units[i:i + 2]:
                start(u.a, u.b)

    def both(*steps):
        for step in steps:
            step()

    rest = (m9, p9, m7, p4, m5, p5)

    def head(is_odd):
        start(m2, p2)
        if not is_odd:
            start(m1[0], p1[0], m1[1], p1[1])
        own_piece(0, 0)
        own_piece(0, 1)
        if not is_odd:
            start(w1[0])
        if is_odd:
            start(g1, h1, g2, h2)
            pl.when(~low)(y1[0].start)
        arrived(m2)
        start(m3)
        arrived(p2)
        start(p3)
        if is_odd:
            start(m1[0], p1[0], m1[1], p1[1])
        else:
            start(m4, p7)
        forward(x1, x2, shards=(0,))
        if is_odd:
            arrived(g1)
            start(g3)
            arrived(h1)
            start(h3)
        for h in (0, 1):
            arrived(m1[h])
            own_piece(3, h)
            arrived(p1[h])
            own_piece(1, h)
        if not is_odd:
            start(w1[3])
            start(*rest)
        arrived(m3)
        own_piece(2, 0)
        arrived(p3)
        own_piece(2, 1)

    def even_core():
        head(False)
        begin(u00)
        forward(w1, w2, shards=(0,))
        forward(x1, x2, shards=(3, 1, 2))
        begin(u10)
        arrived(m4, p7)
        start(p8)
        arrived(p9)
        begin(u01, u11)
        u00.middle()
        arrived(m9, m7)
        start(m8)
        arrived(p4)
        pl.semaphore_signal(gate, inc=1, device_id=gp, device_id_type=MESH)
        u10.middle()
        forward(w1, w2, shards=(3,))
        arrived(x2[0], x2[3])
        begin(u02, u12)
        both(u01.middle, u11.middle)
        forward(x2, x3, shards=(1, 2))
        begin(u20, u21, u22)
        both(u12.middle, u02.middle)
        arrived(m5, p5, m8, p8)
        begin(u03, u13, u23)
        both(u20.middle, u21.middle, u22.middle)
        arrived(*x3)
        begin(u30, u31)
        both(u13.middle, u10.end, u11.end, u00.end, u01.end)
        arrived(*x4)
        begin(u40, u41)
        both(u30.middle, u12.end, u02.end)
        both(u40.middle, u41.middle, u31.middle, u03.middle, u23.middle)
        both(u13.end, u20.end, u21.end, u22.end, u30.end, u40.end, u41.end, u31.end, u03.end, u23.end)

    def pass_on(*shards):
        for r in shards:
            arrived(w2[r] if r in w2 else x3[r])
            x4[r].start()

    def odd_core():
        head(True)
        pl.when(relays)(lambda: forward(y1, y2, shards=(0,)))
        forward(x1, x2, shards=(3, 1))
        arrived(g2)
        pl.when(~low)(y1[3].start)
        arrived(h2)
        pl.when(~low)(y1[1].start)
        arrived(g3, h3)
        pl.when(~low)(y1[2].start)
        pl.semaphore_wait(gate, 1)
        start(m4, p7, *rest)
        forward(x1, x2, shards=(2,))
        begin(u10)
        forward(x2, x3, shards=(0, 3))
        u10.middle()
        forward(x2, x3, shards=(1,))
        arrived(m4, p7)
        start(p8)
        arrived(p9)
        begin(u11)
        pl.when(relays)(lambda: forward(y1, y2, shards=(3,)))
        forward(x2, x3, shards=(2,))
        begin(u20, u21)
        pass_on(0, 3)
        arrived(m9, m7)
        start(m8)
        arrived(p4)
        begin(u12, u22)
        pl.when(relays)(lambda: forward(y1, y2, shards=(1,)))
        both(u11.middle, u20.middle, u21.middle)
        pass_on(1, 2)
        pl.when(relays)(lambda: forward(y1, y2, shards=(2,)))
        arrived(m5, p5, m8, p8)
        begin(u13, u23, u30, u31)
        both(u12.middle)
        begin(v00, v01)

        def last_pair():
            arrived(*y2)
            begin(v40, v41)

        pl.when(low)(last_pair)
        both(u13.middle)
        both(u10.end, u11.end, u20.end, u21.end, v00.middle, v01.middle)
        both(u30.middle, u31.middle, u12.end)
        both(u22.middle, u23.middle)
        pl.when(low)(lambda: both(v40.middle, v41.middle))
        both(u13.end, u30.end, u31.end, v00.end, v01.end, u22.end, u23.end)
        pl.when(low)(lambda: both(v40.end, v41.end))

    pl.when(~odd)(even_core)
    pl.when(odd)(odd_core)
    both(u10.receive, u11.receive, u12.receive, u13.receive, u30.receive, u31.receive)

    @pl.when(low & ~odd)
    def _():
        both(u40.receive, u41.receive)

    @pl.when(~low)
    def _():
        out_ref[4] = jnp.zeros(out_ref.shape[1:], out_ref.dtype)

    left(*m1, *p1, m2, p2, m3, p3, m4, p4, m5, p5, m7, p7, m8, p8, m9, p9, *x2, x3[1], x3[2])
    for r in range(4):
        left(*x1[r])
    for u in always:
        u.settle()

    @pl.when(odd)
    def _():
        left(g1, h1, g2, h2, g3, h3, x3[0], x3[3], *x4)
        for u in odd_only:
            u.settle()

    @pl.when(~odd)
    def _():
        left(w1[0], w1[3], w2[0], w2[3])
        for u in even_only:
            u.settle()

    @pl.when(low & odd)
    def _():
        both(v40.settle, v41.settle)

    @pl.when(~low & ~odd)
    def _():
        left(*u40.sends, *u41.sends)

    pl.when(odd & ~low)(lambda: left(*y1))
    pl.when(relays)(lambda: left(*y2))

def solution(mesh):
    def local_fn(a_blk):
        rows, cols = a_blk.shape
        strip = rows // 16
        out = pl.pallas_call(
            kernel,
            out_shape=jax.ShapeDtypeStruct((5, strip, rows), jnp.float32),
            in_specs=[pl.BlockSpec(memory_space=pltpu.HBM)] * 2,
            out_specs=pl.BlockSpec(memory_space=pltpu.VMEM),
            scratch_shapes=[
                pltpu.VMEM((rows, 4 * cols), jnp.bfloat16),
                pltpu.VMEM((4, 4, strip, 4 * cols), jnp.bfloat16),
                pltpu.VMEM((4, rows // 4, 4 * cols), jnp.bfloat16),
                pltpu.VMEM((2, 4, strip, 4 * cols), jnp.bfloat16),
                pltpu.VMEM((rows // 4, 2 * cols), jnp.bfloat16),
                pltpu.VMEM((5, rows // 4, rows), jnp.float32),
                pltpu.VMEM((2, 5, strip, rows // 2), jnp.float32),
                pltpu.VMEM((2, 5, strip, rows), jnp.float32),
                pltpu.VMEM((3, strip, rows), jnp.float32),
                pltpu.VMEM((3, strip, rows), jnp.float32),
                pltpu.SemaphoreType.DMA((220,)),
                pltpu.SemaphoreType.DMA((220,)),
                pltpu.SemaphoreType.DMA,
                pltpu.SemaphoreType.DMA,
                pltpu.SemaphoreType.REGULAR,
            ],
            compiler_params=pltpu.CompilerParams(
                collective_id=0, has_side_effects=True, vmem_limit_bytes=48 * 1024 * 1024),
        )(pltpu.with_memory_space_constraint(a_blk, pltpu.HBM),
          pltpu.with_memory_space_constraint(a_blk.reshape(4, 4, strip, cols), pltpu.HBM))
        return out[None]

    return jax.shard_map(local_fn, mesh=mesh, in_specs=(P(("m", "g"), "kk"),), out_specs=P(("m", "g"), None, "kk", None), check_vma=False)
```
